64 devices in a mesh: dp: 4 (over x, y), cp: 16 (over z, core).
Axes of the slice: x: 2, y: 2, z: 8, core: 2. Of those that a mesh axis runs over, the one named last changes fastest.
The devices are a block of a 4x4x8 slice.
Arguments:
- queries: bfloat16 [1536, 64, 128], P(('dp', 'cp')), parts along dimension 0
- key_new: bfloat16 [1536, 8, 128], P(('dp', 'cp')), parts along dimension 0
- value_new: bfloat16 [1536, 8, 128], P(('dp', 'cp')), parts along dimension 0
- key_cache: bfloat16 [131072, 8, 128], P(('dp', 'cp')), parts along dimension 0
- value_cache: bfloat16 [131072, 8, 128], P(('dp', 'cp')), parts along dimension 0
- prefix_len: int32 [4], P('dp'), parts along dimension 0
Outputs:
- output 1: bfloat16 [1536, 64, 128], P(('dp', 'cp')), parts along dimension 0
- output 2: float32 [1536, 64], P(('dp', 'cp')), parts along dimension 0
There are 4 independent parts. The reference program is written for one: setup_inputs(seed, part) draws one part's arguments, and reference() takes and returns one part's arrays. A program takes and returns all parts, laid end to end along the dimension named above; each array names one.
All inputs are finite; a program needn't handle non-finite values.
Results may differ from the reference program's by a relative error of at most 0.00914856.
Values are sent between devices in bfloat16 or wider.
A program may use at most 768 MiB of HBM per device.

```python
import math
import jax
import jax.numpy as jnp
from jax import lax

GROUP_SIZE = 16
NEW_DEV = 24
PREFIX_DEV = 2048
Q_HEADS = 64
KV_HEADS = 8
HEAD_DIM = 128
NEW_LEN = GROUP_SIZE * NEW_DEV
P_MAX = GROUP_SIZE * PREFIX_DEV
GROUP_RATIO = Q_HEADS // KV_HEADS


def setup_inputs(seed: int = 0, part: int = 0) -> dict:
    base_key = jax.random.fold_in(jax.random.key(seed), part)
    rand_keys = jax.random.split(base_key, 9)
    shift_scale = GROUP_SIZE ** 0.5
    new_boost = math.log(P_MAX / NEW_LEN) * 2.0 ** 0.5
    direction = jax.random.normal(rand_keys[0], (KV_HEADS, HEAD_DIM), jnp.float32)
    direction = direction / jnp.linalg.norm(direction, axis=-1, keepdims=True)
    q_mean = jnp.repeat(direction, GROUP_RATIO, axis=0) * HEAD_DIM ** 0.5
    q_noise = jax.random.normal(rand_keys[1], (NEW_LEN, Q_HEADS, HEAD_DIM), jnp.float32)
    queries = (q_noise + q_mean[None]) * 0.5 ** 0.5
    key_new = jax.random.normal(rand_keys[2], (NEW_LEN, KV_HEADS, HEAD_DIM), jnp.float32) + new_boost * direction[None]
    new_shift = jax.random.normal(rand_keys[3], (GROUP_SIZE, 1, KV_HEADS, HEAD_DIM), jnp.float32) * shift_scale
    value_new = jax.random.normal(rand_keys[4], (GROUP_SIZE, NEW_DEV, KV_HEADS, HEAD_DIM), jnp.float32) + new_shift
    key_cache = jax.random.normal(rand_keys[5], (P_MAX, KV_HEADS, HEAD_DIM), jnp.float32)
    cache_shift = jax.random.normal(rand_keys[6], (GROUP_SIZE, 1, KV_HEADS, HEAD_DIM), jnp.float32) * shift_scale
    value_cache = jax.random.normal(rand_keys[7], (GROUP_SIZE, PREFIX_DEV, KV_HEADS, HEAD_DIM), jnp.float32) + cache_shift
    prefix_len = jax.random.randint(rand_keys[8], (1,), (3 * P_MAX) // 4, P_MAX + 1, jnp.int32)
    return {
        'queries': queries.astype(jnp.bfloat16),
        'key_new': key_new.astype(jnp.bfloat16),
        'value_new': value_new.reshape(NEW_LEN, KV_HEADS, HEAD_DIM).astype(jnp.bfloat16),
        'key_cache': key_cache.astype(jnp.bfloat16),
        'value_cache': value_cache.reshape(P_MAX, KV_HEADS, HEAD_DIM).astype(jnp.bfloat16),
        'prefix_len': prefix_len,
    }


def reference(queries, key_new, value_new, key_cache, value_cache, prefix_len):
    prefix_end = prefix_len[0]
    key_pos = jnp.arange(P_MAX + NEW_LEN)
    logit_scale = HEAD_DIM ** -0.5

    def one_head(head_idx):
        kv_idx = head_idx // GROUP_RATIO
        keys_all = jnp.concatenate([lax.dynamic_index_in_dim(key_cache, kv_idx, axis=1, keepdims=False), lax.dynamic_index_in_dim(key_new, kv_idx, axis=1, keepdims=False)], axis=0).astype(jnp.float32)
        vals_all = jnp.concatenate([lax.dynamic_index_in_dim(value_cache, kv_idx, axis=1, keepdims=False), lax.dynamic_index_in_dim(value_new, kv_idx, axis=1, keepdims=False)], axis=0).astype(jnp.float32)
        q_head = lax.dynamic_index_in_dim(queries, head_idx, axis=1, keepdims=False).astype(jnp.float32).reshape(GROUP_SIZE, NEW_DEV, HEAD_DIM)

        def one_block(block_args):
            q_rows, row_start = block_args
            scores = jnp.dot(q_rows, keys_all.T) * logit_scale
            q_pos = row_start + jnp.arange(NEW_DEV)
            visible = jnp.where(key_pos[None, :] < P_MAX, key_pos[None, :] < prefix_end, key_pos[None, :] - P_MAX <= q_pos[:, None])
            scores = jnp.where(visible, scores, -jnp.inf)
            row_max = jnp.max(scores, axis=-1)
            exp_scores = jnp.exp(scores - row_max[:, None])
            row_sum = jnp.sum(exp_scores, axis=-1)
            prob_bf = exp_scores.astype(jnp.bfloat16).astype(jnp.float32)
            block_out = jnp.dot(prob_bf, vals_all) / row_sum[:, None]
            return block_out.astype(jnp.bfloat16), row_max + jnp.log(row_sum)

        head_out, head_lse = lax.map(one_block, (q_head, jnp.arange(GROUP_SIZE) * NEW_DEV))
        return head_out.reshape(NEW_LEN, HEAD_DIM), head_lse.reshape(NEW_LEN)

    all_out, all_lse = lax.map(one_head, jnp.arange(Q_HEADS))
    return jnp.transpose(all_out, (1, 0, 2)), jnp.transpose(all_lse)
```

```python
import functools

import jax
import jax.numpy as jnp
from jax import lax
from jax.experimental import pallas as pl
from jax.experimental.pallas import tpu as pltpu
from jax.sharding import PartitionSpec as P

NEG = -1e30
LOG2E = 1.4426950408889634
F32 = jnp.float32
BF16 = jnp.bfloat16
TILE = 256
NEW_PAD = 32
SUB = 2048


def _attend(nz, tok, heads, ratio, cache,
            q_hbm, kt_hbm, vt_hbm, kn_hbm, vn_hbm, plen_ref, out_hbm, lse_hbm,
            kbuf, vbuf, knbuf, vnbuf, qbuf, s0, s1, sn0, sn1, bias, qt0, qt1,
            po, plse, rb, rl, outb, lseb,
            kv_loc, kv_send, kv_recv, kn_sem, q_loc, q_send, q_recv,
            ag_send, ag_recv, ro_send, ro_recv, rs_send, rs_recv, out_sem, fin_sem):
    hd = q_hbm.shape[-1]
    scale = hd ** -0.5
    csc = scale * LOG2E
    half = nz // 2
    rows = 2 * tok * ratio
    mine = tok * ratio
    keys = 2 * cache
    per_step = 2 * rows // TILE
    steps = heads * half
    tiles = steps * per_step
    bodies = (tiles + 2) // 2

    rank = lax.axis_index("cp")
    z, c = rank // 2, rank % 2
    partner = 2 * z + (1 - c)
    right = 2 * lax.rem(z + 1, nz) + c
    left = 2 * lax.rem(z + nz - 1, nz) + c
    to = (right, left)

    barrier = pltpu.get_barrier_semaphore()
    for dev in (partner, right, left):
        pl.semaphore_signal(barrier, inc=1, device_id={"cp": dev}, device_id_type=pl.DeviceIdType.MESH)
    pl.semaphore_wait(barrier, 3)

    def remote(src, dst, ss, rs, dev):
        return pltpu.make_async_remote_copy(src_ref=src, dst_ref=dst, send_sem=ss, recv_sem=rs,
                                            device_id={"cp": dev}, device_id_type=pl.DeviceIdType.MESH)

    def q_in(h):
        there = remote(q_hbm.at[heads * (1 - c) + h], qbuf.at[h, 0, pl.ds(c * mine, mine)], q_send.at[h], q_recv.at[h], partner)
        here = pltpu.make_async_copy(q_hbm.at[heads * c + h], qbuf.at[h, 0, pl.ds(c * mine, mine)], q_loc.at[h])
        return there, here

    def kv_in(h):
        out = []
        for n, (src, dst) in enumerate(((kt_hbm, kbuf.at[h, pl.ds(c * cache, cache), :]),
                                        (vt_hbm, vbuf.at[h, :, pl.ds(c * cache, cache)]))):
            out.append((remote(src.at[heads * (1 - c) + h], dst, kv_send.at[n, h], kv_recv.at[n, h], partner),
                        pltpu.make_async_copy(src.at[heads * c + h], dst, kv_loc.at[n, h])))
        return out

    def new_in():
        out = []
        for n, (src, dst) in enumerate(((kn_hbm, knbuf), (vn_hbm, vnbuf))):
            out.append((remote(src.at[pl.ds(heads * (1 - c), heads)], dst.at[c], kn_sem.at[n, 0], kn_sem.at[n, 1], partner),
                        pltpu.make_async_copy(src.at[pl.ds(heads * c, heads)], dst.at[c], kn_sem.at[n, 2])))
        return out

    def q_slot(h, d, k):
        if k == 0:
            return qbuf.at[h, 0, pl.ds(0, rows)]
        if k == half:
            return qbuf.at[h, 0, pl.ds(rows, rows)]
        return qbuf.at[h, k, pl.ds(d * rows, rows)]

    def far_dir(h):
        return h % 2

    def ag(h, d, k):
        return remote(q_slot(h, d, k), q_slot(h, d, k + 1), ag_send.at[d, h, k], ag_recv.at[d, h, k], to[d])

    def ag_start(h, k):
        for d in (0, 1):
            if k + 1 < half or far_dir(h) == d:
                ag(h, d, k).start()

    def ag_wait(h, k):
        for d in (0, 1):
            if k + 1 < half or far_dir(h) == d:
                ag(h, d, k).wait_recv()

    def po_part(h, d, k):
        if k == half:
            sl = pl.ds(rows, rows)
            return po.at[h, 0, :, sl], plse.at[h, 0, :, sl]
        sl = pl.ds((1 - d) * rows, rows)
        return po.at[h, k, :, sl], plse.at[h, k, :, sl]

    def rs(h, d, k):
        o, l = po_part(h, d, k)
        return (remote(o, rb.at[d, h, k - 1], ro_send.at[d, h, k - 1], ro_recv.at[d, h, k - 1], to[d]),
                remote(l, rl.at[d, h, k - 1], rs_send.at[d, h, k - 1], rs_recv.at[d, h, k - 1], to[d]))

    def merge(parts):
        top = functools.reduce(jnp.maximum, [l for _, l in parts])
        ws = [jnp.exp(l - top) for _, l in parts]
        tot = functools.reduce(jnp.add, ws)
        inv = 1.0 / tot
        acc = functools.reduce(jnp.add, [o.astype(F32) * (w * inv) for (o, _), w in zip(parts, ws)])
        return acc, top + jnp.log(tot)

    def rs_stage(h, k):
        for d in (0, 1):
            if k == half and far_dir(h) != d:
                continue
            if k + 1 < half or (k + 1 == half and far_dir(h) == d):
                for cp in rs(h, d, k + 1):
                    cp.wait_recv()
                o, l = po_part(h, d, k)
                acc, lse = merge([(o[...], l[...]), (rb[d, h, k], rl[d, h, k])])
                o[...] = acc.astype(BF16)
                l[...] = lse
            for cp in rs(h, d, k):
                cp.start()

    def out_copies(h):
        there = remote(outb.at[h, pl.ds((1 - c) * mine, mine)], out_hbm.at[heads * c + h], out_sem.at[h, 0], out_sem.at[h, 1], partner)
        here = pltpu.make_async_copy(outb.at[h, pl.ds(c * mine, mine)], out_hbm.at[heads * c + h], out_sem.at[h, 2])
        return there, here

    def final(h):
        for d in (0, 1):
            for cp in rs(h, d, 1):
                cp.wait_recv()
        acc, lse = merge([(po[h, 0, :, 0:rows], plse[h, 0, :, 0:rows])] + [(rb[d, h, 0], rl[d, h, 0]) for d in (0, 1)])
        outb[h] = acc.T.astype(BF16)
        lseb[h:h + 1, :] = lse
        for cp in out_copies(h):
            cp.start()

    def kv_wait(h):
        for there, here in kv_in(h):
            here.wait()
            there.wait_recv()

    for h in range(heads):
        for cp in q_in(h):
            cp.start()
    for there, here in kv_in(0) + new_in():
        there.start()
        here.start()
    for h in range(1, heads):
        for there, here in kv_in(h):
            there.start()
            here.start()

    def q_wait_send(h):
        there, here = q_in(h)
        here.wait()
        there.wait_recv()
        ag_start(h, 0)

    pos = z * keys + lax.broadcasted_iota(jnp.int32, (keys, hd), 0)
    lane = lax.broadcasted_iota(jnp.int32, (keys, hd), 1)
    bias[...] = jnp.where((pos >= plen_ref[0]) & (lane == 0), NEG, 0.0).astype(BF16)
    ones = jnp.where(lax.broadcasted_iota(jnp.int32, (TILE - hd, TILE), 0) == 0, 1.0, 0.0).astype(BF16)
    for r in (qt0, qt1):
        r[hd:TILE, :] = ones
    lseb[...] = jnp.zeros_like(lseb)
    QT, SR, SN = (qt0, qt1), (s0, s1), (sn0, sn1)

    for h in (0, 1):
        q_wait_send(h)

    ev = {i: [] for i in range(bodies + 1)}

    def at(i, f, *a):
        ev[min(i, bodies)].append((f, a))

    def need(s):
        return (3 * s - 1) // 2

    def hop(h, k):
        ag_wait(h, k)
        if k + 1 < half:
            ag_start(h, k + 1)

    for k in range(half):
        at((0, 1, 2, 4)[k], hop, 0, k)
    for k in range(half):
        at((1, 2, 4, 5)[k], hop, 1, k)
    at(3, q_wait_send, 2)
    for k in range(half):
        at((5, 7, 9, 11)[k], hop, 2, k)
    at(9, q_wait_send, 3)
    for k in range(half):
        at((11, 13, 15, 17)[k], hop, 3, k)
    for h in range(1, heads):
        at(6 * h, kv_wait, h)
    for h, when in enumerate(((7, 9, 11, 13, 15), (9, 11, 13, 15, 17), (15, 17, 19, 21, 23), (21, 23, 24, 25, 25))):
        for j, k in enumerate(range(half, 0, -1)):
            at(when[j], rs_stage, h, k)
        at(when[half], final, h)

    def place(t):
        s, n = t // per_step, lax.rem(t, per_step)
        h, r = s // half, lax.rem(s, half)
        pair = jnp.where(h == 0, lax.rem(r + 1, half), lax.rem(half - r, half))
        return h, pair, n

    def make_qt(t, slot):
        h, pair, n = place(jnp.clip(t, 0, tiles - 1))
        q = qbuf[h, pair, pl.ds(pl.multiple_of(n * TILE, TILE), TILE), :]
        QT[slot][0:hd, :] = q.astype(F32).T.astype(BF16)

    def dot(a, b):
        return lax.dot_general(a, b, (((1,), (0,)), ((), ())), preferred_element_type=F32)

    def colmax(x):
        return jnp.max(x.reshape(x.shape[0] // 8, 8, TILE), axis=0)

    def colsum(x):
        return jnp.sum(x.reshape(x.shape[0] // 8, 8, TILE), axis=0)

    def tile(i, mm, par):
        hA, pairA, nA = place(jnp.clip(i + 1, 0, tiles - 1))
        hB, pairB, nB = place(jnp.clip(i, 0, tiles - 1))
        m = jnp.max(mm, axis=0, keepdims=True)
        mc = m * csc
        l = jnp.zeros((8, TILE), F32)
        mm = jnp.full((8, TILE), -jnp.inf, F32)
        acc = None
        for u in range(keys // SUB):
            sl = pl.ds(u * SUB, SUB)
            sv = dot(jnp.concatenate([kbuf[hA, sl, :], bias[sl, :]], axis=1), QT[par][...])
            SR[par][sl, :] = sv
            mm = jnp.maximum(mm, colmax(sv))
            pe = jnp.exp2(SR[1 - par][sl, :] * csc - mc)
            l = l + colsum(pe)
            pv = dot(vbuf[hB, :, sl], pe.astype(BF16))
            acc = pv if acc is None else acc + pv
            if u == 0:
                make_qt(i + 2, 1 - par)
        blk_a = jnp.where(pairA == 0, z, lax.rem(z + nz - pairA, nz))
        blk_b = jnp.where(pairA == 0, lax.rem(z + half, nz), lax.rem(z + pairA, nz))
        tl = (nA * TILE + lax.broadcasted_iota(jnp.int32, (NEW_PAD, TILE), 1)) // ratio
        qtok = jnp.where(tl < 2 * tok, 2 * tok * blk_a + tl, 2 * tok * blk_b + tl - 2 * tok)
        kid = lax.broadcasted_iota(jnp.int32, (NEW_PAD, TILE), 0)
        pn = []
        for q in (0, 1):
            pe = jnp.exp2(SN[1 - par][q] * csc - mc)
            l = l + colsum(pe)
            pn += [pe.astype(BF16), jnp.zeros((128 - NEW_PAD, TILE), BF16)]
            ktok = 2 * tok * z + tok * q + kid
            sv = jnp.where((kid < tok) & (ktok <= qtok), dot(knbuf[q, hA], QT[par][0:hd, :]), NEG)
            SN[par][q] = sv
            mm = jnp.maximum(mm, colmax(sv))
        acc = acc + dot(jnp.concatenate([vnbuf[0, hB], vnbuf[1, hB]], axis=1), jnp.concatenate(pn, axis=0))
        lt = jnp.sum(l, axis=0, keepdims=True)
        sl = pl.ds(pl.multiple_of(nB * TILE, TILE), TILE)
        plse[hB, pairB, :, sl] = m * scale + jnp.log(lt)
        po[hB, pairB, :, sl] = (acc * (1.0 / lt)).astype(BF16)
        return mm

    for f, a in ev[0]:
        f(*a)
    kv_wait(0)
    for there, here in new_in():
        here.wait()
        there.wait_recv()
    make_qt(0, 0)

    def pair_of_tiles(t, mm):
        for i in range(1, bodies):
            if ev[i]:
                @pl.when(t == i)
                def _(i=i):
                    for f, a in ev[i]:
                        f(*a)
        return tile(2 * t, tile(2 * t - 1, mm, 0), 1)

    lax.fori_loop(0, bodies, pair_of_tiles, jnp.zeros((8, TILE), F32))

    for f, a in ev[bodies]:
        f(*a)
    fin = (remote(lseb, lse_hbm.at[c], fin_sem.at[0], fin_sem.at[1], partner),
           pltpu.make_async_copy(lseb, lse_hbm.at[c], fin_sem.at[2]))
    for cp in fin:
        cp.start()

    for h in range(heads):
        q_in(h)[0].wait_send()
        for there, _ in kv_in(h):
            there.wait_send()
        for d in (0, 1):
            for k in range(half):
                if k + 1 < half or far_dir(h) == d:
                    ag(h, d, k).wait_send()
            for k in range(1, half + 1):
                if k < half or far_dir(h) == d:
                    for cp in rs(h, d, k):
                        cp.wait_send()
        there, here = out_copies(h)
        here.wait()
        there.wait()
    for there, _ in new_in():
        there.wait_send()
    fin[1].wait()
    fin[0].wait()


def solution(mesh):
    nz = mesh.shape["cp"] // 2
    tok_spec = P(("dp", "cp"))

    def local(queries, key_new, value_new, key_cache, value_cache, prefix_len):
        tok, nq, hd = queries.shape
        cache, nkv = key_cache.shape[0], key_cache.shape[1]
        ratio = nq // nkv
        heads = nkv // 2
        half = nz // 2
        rank = lax.axis_index("cp")
        c = rank % 2
        ok = (rank * cache + jnp.arange(cache) < prefix_len[0])[:, None, None]
        zero = jnp.zeros((), BF16)
        kt = jnp.where(ok, key_cache, zero).transpose(1, 0, 2)
        vt = jnp.where(ok, value_cache, zero).transpose(1, 2, 0)
        kn = jnp.pad(key_new.transpose(1, 0, 2), ((0, 0), (0, NEW_PAD - tok), (0, 0)))
        vn = jnp.pad(value_new.transpose(1, 2, 0), ((0, 0), (0, 0), (0, 128 - tok)))
        qh = queries.reshape(tok, nkv, ratio, hd).transpose(1, 0, 2, 3).reshape(nkv, tok * ratio, hd)
        rows, mine, keys = 2 * tok * ratio, tok * ratio, 2 * cache
        dma = pltpu.SemaphoreType.DMA
        out, lse = pl.pallas_call(
            functools.partial(_attend, nz, tok, heads, ratio, cache),
            out_shape=(jax.ShapeDtypeStruct((nkv, mine, hd), BF16), jax.ShapeDtypeStruct((2, 8, rows), F32)),
            in_specs=[pl.BlockSpec(memory_space=pl.ANY)] * 5 + [pl.BlockSpec(memory_space=pltpu.SMEM)],
            out_specs=[pl.BlockSpec(memory_space=pl.ANY)] * 2,
            scratch_shapes=[
                pltpu.VMEM((heads, keys, hd), BF16), pltpu.VMEM((heads, hd, keys), BF16),
                pltpu.VMEM((2, heads, NEW_PAD, hd), BF16), pltpu.VMEM((2, heads, hd, 128), BF16),
                pltpu.VMEM((heads, half, 2 * rows, hd), BF16),
                pltpu.VMEM((keys, TILE), F32), pltpu.VMEM((keys, TILE), F32),
                pltpu.VMEM((2, NEW_PAD, TILE), F32), pltpu.VMEM((2, NEW_PAD, TILE), F32),
                pltpu.VMEM((keys, hd), BF16),
                pltpu.VMEM((TILE, TILE), BF16), pltpu.VMEM((TILE, TILE), BF16),
                pltpu.VMEM((heads, half, hd, 2 * rows), BF16), pltpu.VMEM((heads, half, 1, 2 * rows), F32),
                pltpu.VMEM((2, heads, half, hd, rows), BF16), pltpu.VMEM((2, heads, half, 1, rows), F32),
                pltpu.VMEM((heads, rows, hd), BF16), pltpu.VMEM((8, rows), F32),
                dma((2, heads)), dma((2, heads)), dma((2, heads)), dma((2, 3)),
                dma((heads,)), dma((heads,)), dma((heads,)),
                dma((2, heads, half)), dma((2, heads, half)),
                dma((2, heads, half)), dma((2, heads, half)),
                dma((2, heads, half)), dma((2, heads, half)),
                dma((heads, 3)), dma((3,)),
            ],
            compiler_params=pltpu.CompilerParams(collective_id=0, has_side_effects=True, vmem_limit_bytes=60 * 2**20),
            name="ring_attend",
        )(qh, kt, vt, kn, vn, prefix_len)
        attn = out.reshape(nkv, tok, ratio, hd).transpose(1, 0, 2, 3).reshape(tok, nq, hd)
        lse = lse[:, :heads].reshape(nkv, 2, tok, ratio)
        lse = lax.dynamic_index_in_dim(lse, c, axis=1, keepdims=False)
        row_lse = lse.transpose(1, 0, 2).reshape(tok, nq)
        return attn, row_lse

    return jax.shard_map(local, mesh=mesh, in_specs=(tok_spec,) * 5 + (P("dp"),), out_specs=(tok_spec, tok_spec), check_vma=False)
```

```python
import functools

import jax
import jax.numpy as jnp
from jax import lax
from jax.experimental import pallas as pl
from jax.experimental.pallas import tpu as pltpu
from jax.sharding import PartitionSpec as P

NEG = -1e30
LOG2E = 1.4426950408889634
F32 = jnp.float32
BF16 = jnp.bfloat16
TILE = 256
NEW_PAD = 32
SUB = 2048
CHUNK = 256


def _attend(nz, tok, heads, ratio, cache,
            q_hbm, k_hbm, v_hbm, kn_hbm, vn_hbm, plen_ref, out_hbm, lse_hbm,
            kbuf, vbuf, knbuf, vnbuf, qbuf, s0, s1, sn0, sn1, bias, qt0, qt1,
            po, plse, rb, rl, outb, lseb, rawk, rawv, st, ksend, vsend,
            raw_sem, kv_send, kv_recv, kn_sem, q_loc, q_send, q_recv,
            ag_send, ag_recv, ro_send, ro_recv, rs_send, rs_recv, out_sem, fin_sem):
    hd = q_hbm.shape[-1]
    scale = hd ** -0.5
    csc = scale * LOG2E
    half = nz // 2
    rows = 2 * tok * ratio
    mine = tok * ratio
    keys = 2 * cache
    per_step = 2 * rows // TILE
    steps = heads * half
    tiles = steps * per_step
    bodies = (tiles + 2) // 2

    rank = lax.axis_index("cp")
    z, c = rank // 2, rank % 2
    partner = 2 * z + (1 - c)
    right = 2 * lax.rem(z + 1, nz) + c
    left = 2 * lax.rem(z + nz - 1, nz) + c
    to = (right, left)

    barrier = pltpu.get_barrier_semaphore()
    for dev in (partner, right, left):
        pl.semaphore_signal(barrier, inc=1, device_id={"cp": dev}, device_id_type=pl.DeviceIdType.MESH)
    pl.semaphore_wait(barrier, 3)

    def remote(src, dst, ss, rs, dev):
        return pltpu.make_async_remote_copy(src_ref=src, dst_ref=dst, send_sem=ss, recv_sem=rs,
                                            device_id={"cp": dev}, device_id_type=pl.DeviceIdType.MESH)

    def head_rows(ref, n):
        return ref.at[:, pl.ds(pl.multiple_of(n * ratio, ratio), ratio), :]

    def q_in(h):
        dst = qbuf.at[h, 0, pl.ds(c * tok, tok)]
        there = remote(head_rows(q_hbm, heads * (1 - c) + h), dst, q_send.at[h], q_recv.at[h], partner)
        here = pltpu.make_async_copy(head_rows(q_hbm, heads * c + h), dst, q_loc.at[h])
        return there, here

    def raw_in():
        return [pltpu.make_async_copy(src, dst, raw_sem.at[n]) for n, (src, dst) in enumerate(((k_hbm, rawk), (v_hbm, rawv)))]

    def kv_in(h):
        return [remote(ksend.at[h], kbuf.at[h, pl.ds(c * cache, cache), :], kv_send.at[0, h], kv_recv.at[0, h], partner),
                remote(vsend.at[h], vbuf.at[h, :, pl.ds(c * cache, cache)], kv_send.at[1, h], kv_recv.at[1, h], partner)]

    def relayout(raw, put):
        def chunk(i, _):
            st[...] = raw[pl.ds(pl.multiple_of(i * CHUNK * 2 * heads, CHUNK * 2 * heads), CHUNK * 2 * heads), :].astype(F32)
            ok = rank * cache + i * CHUNK + lax.broadcasted_iota(jnp.int32, (CHUNK, hd), 0) < plen_ref[0]
            at0 = pl.multiple_of(i * CHUNK, CHUNK)
            for h in range(heads):
                for own, n in ((True, heads * c + h), (False, heads * (1 - c) + h)):
                    put(own, h, at0, jnp.where(ok, st[pl.ds(n, CHUNK, stride=2 * heads), :], 0.0))
            return 0
        lax.fori_loop(0, cache // CHUNK, chunk, 0)

    def put_k(own, h, at0, x):
        if own:
            kbuf[h, pl.ds(pl.multiple_of(c * cache + at0, CHUNK), CHUNK), :] = x.astype(BF16)
        else:
            ksend[h, pl.ds(at0, CHUNK), :] = x.astype(BF16)

    def put_v(own, h, at0, x):
        if own:
            vbuf[h, :, pl.ds(pl.multiple_of(c * cache + at0, CHUNK), CHUNK)] = x.T.astype(BF16)
        else:
            vsend[h, :, pl.ds(at0, CHUNK)] = x.T.astype(BF16)

    def new_in():
        out = []
        for n, (src, dst) in enumerate(((kn_hbm, knbuf), (vn_hbm, vnbuf))):
            out.append((remote(src.at[pl.ds(heads * (1 - c), heads)], dst.at[c], kn_sem.at[n, 0], kn_sem.at[n, 1], partner),
                        pltpu.make_async_copy(src.at[pl.ds(heads * c, heads)], dst.at[c], kn_sem.at[n, 2])))
        return out

    def q_slot(h, d, k):
        if k == 0:
            return qbuf.at[h, 0, pl.ds(0, 2 * tok)]
        if k == half:
            return qbuf.at[h, 0, pl.ds(2 * tok, 2 * tok)]
        return qbuf.at[h, k, pl.ds(d * 2 * tok, 2 * tok)]

    def far_dir(h):
        return h % 2

    def ag(h, d, k):
        return remote(q_slot(h, d, k), q_slot(h, d, k + 1), ag_send.at[d, h, k], ag_recv.at[d, h, k], to[d])

    def ag_start(h, k):
        for d in (0, 1):
            if k + 1 < half or far_dir(h) == d:
                ag(h, d, k).start()

    def ag_wait(h, k):
        for d in (0, 1):
            if k + 1 < half or far_dir(h) == d:
                ag(h, d, k).wait_recv()

    def hop(h, k):
        ag_wait(h, k)
        if k + 1 < half:
            ag_start(h, k + 1)

    def po_part(h, d, k):
        if k == half:
            sl = pl.ds(rows, rows)
            return po.at[h, 0, :, sl], plse.at[h, 0, :, sl]
        sl = pl.ds((1 - d) * rows, rows)
        return po.at[h, k, :, sl], plse.at[h, k, :, sl]

    def rs(h, d, k):
        o, l = po_part(h, d, k)
        return (remote(o, rb.at[d, h, k - 1], ro_send.at[d, h, k - 1], ro_recv.at[d, h, k - 1], to[d]),
                remote(l, rl.at[d, h, k - 1], rs_send.at[d, h, k - 1], rs_recv.at[d, h, k - 1], to[d]))

    def merge(parts):
        top = functools.reduce(jnp.maximum, [l for _, l in parts])
        ws = [jnp.exp(l - top) for _, l in parts]
        tot = functools.reduce(jnp.add, ws)
        inv = 1.0 / tot
        acc = functools.reduce(jnp.add, [o.astype(F32) * (w * inv) for (o, _), w in zip(parts, ws)])
        return acc, top + jnp.log(tot)

    def rs_stage(h, k):
        for d in (0, 1):
            if k == half and far_dir(h) != d:
                continue
            if k + 1 < half or (k + 1 == half and far_dir(h) == d):
                for cp in rs(h, d, k + 1):
                    cp.wait_recv()
                o, l = po_part(h, d, k)
                acc, lse = merge([(o[...], l[...]), (rb[d, h, k], rl[d, h, k])])
                o[...] = acc.astype(BF16)
                l[...] = lse
            for cp in rs(h, d, k):
                cp.start()

    def out_copies(h):
        dst = head_rows(out_hbm, heads * c + h)
        there = remote(outb.at[h, pl.ds((1 - c) * tok, tok)], dst, out_sem.at[h, 0], out_sem.at[h, 1], partner)
        here = pltpu.make_async_copy(outb.at[h, pl.ds(c * tok, tok)], dst, out_sem.at[h, 2])
        return there, here

    def final(h):
        for d in (0, 1):
            for cp in rs(h, d, 1):
                cp.wait_recv()
        acc, lse = merge([(po[h, 0, :, 0:rows], plse[h, 0, :, 0:rows])] + [(rb[d, h, 0], rl[d, h, 0]) for d in (0, 1)])
        outb[h] = acc.T.reshape(2 * tok, ratio, hd).astype(BF16)
        lseb[h:h + 1, :] = lse
        for cp in out_copies(h):
            cp.start()

    def kv_wait(h):
        for there in kv_in(h):
            there.wait_recv()

    for h in range(heads):
        for cp in q_in(h):
            cp.start()
    for cp in raw_in():
        cp.start()
    for there, here in new_in():
        there.start()
        here.start()

    def q_wait_send(h):
        there, here = q_in(h)
        here.wait()
        there.wait_recv()
        ag_start(h, 0)

    pos = z * keys + lax.broadcasted_iota(jnp.int32, (keys, hd), 0)
    lane = lax.broadcasted_iota(jnp.int32, (keys, hd), 1)
    bias[...] = jnp.where((pos >= plen_ref[0]) & (lane == 0), NEG, 0.0).astype(BF16)
    ones = jnp.where(lax.broadcasted_iota(jnp.int32, (TILE - hd, TILE), 0) == 0, 1.0, 0.0).astype(BF16)
    for r in (qt0, qt1):
        r[hd:TILE, :] = ones
    lseb[...] = jnp.zeros_like(lseb)
    QT, SR, SN = (qt0, qt1), (s0, s1), (sn0, sn1)

    for h in (0, 1):
        q_wait_send(h)
    raw_in()[0].wait()
    relayout(rawk, put_k)
    for h in range(heads):
        kv_in(h)[0].start()
    hop(0, 0)
    raw_in()[1].wait()
    relayout(rawv, put_v)
    for h in range(heads):
        kv_in(h)[1].start()

    ev = {i: [] for i in range(bodies + 1)}

    def at(i, f, *a):
        ev[min(i, bodies)].append((f, a))

    def need(s):
        return (3 * s - 1) // 2

    for k in range(1, half):
        at((0, 1, 2, 4)[k], hop, 0, k)
    for k in range(half):
        at((1, 2, 4, 5)[k], hop, 1, k)
    at(3, q_wait_send, 2)
    for k in range(half):
        at((5, 7, 9, 11)[k], hop, 2, k)
    at(9, q_wait_send, 3)
    for k in range(half):
        at((11, 13, 15, 17)[k], hop, 3, k)
    for h in range(1, heads):
        at(6 * h, kv_wait, h)
    for h, when in enumerate(((7, 9, 11, 13, 15), (9, 11, 13, 15, 17), (15, 17, 19, 21, 23), (21, 23, 24, 25, 25))):
        for j, k in enumerate(range(half, 0, -1)):
            at(when[j], rs_stage, h, k)
        at(when[half], final, h)

    def place(t):
        s, n = t // per_step, lax.rem(t, per_step)
        h, r = s // half, lax.rem(s, half)
        pair = jnp.where(h == 0, lax.rem(r + 1, half), lax.rem(half - r, half))
        return h, pair, n

    def make_qt(t, slot):
        h, pair, n = place(jnp.clip(t, 0, tiles - 1))
        q = qbuf[h, pair, pl.ds(n * (TILE // ratio), TILE // ratio)].astype(F32).reshape(TILE, hd)
        QT[slot][0:hd, :] = q.T.astype(BF16)

    def dot(a, b):
        return lax.dot_general(a, b, (((1,), (0,)), ((), ())), preferred_element_type=F32)

    def colmax(x):
        return jnp.max(x.reshape(x.shape[0] // 8, 8, TILE), axis=0)

    def colsum(x):
        return jnp.sum(x.reshape(x.shape[0] // 8, 8, TILE), axis=0)

    def tile(i, mm, par):
        hA, pairA, nA = place(jnp.clip(i + 1, 0, tiles - 1))
        hB, pairB, nB = place(jnp.clip(i, 0, tiles - 1))
        m = jnp.max(mm, axis=0, keepdims=True)
        mc = m * csc
        l = jnp.zeros((8, TILE), F32)
        mm = jnp.full((8, TILE), -jnp.inf, F32)
        acc = None
        for u in range(keys // SUB):
            sl = pl.ds(u * SUB, SUB)
            sv = dot(jnp.concatenate([kbuf[hA, sl, :], bias[sl, :]], axis=1), QT[par][...])
            SR[par][sl, :] = sv
            mm = jnp.maximum(mm, colmax(sv))
            pe = jnp.exp2(SR[1 - par][sl, :] * csc - mc)
            l = l + colsum(pe)
            pv = dot(vbuf[hB, :, sl], pe.astype(BF16))
            acc = pv if acc is None else acc + pv
            if u == 0:
                make_qt(i + 2, 1 - par)
        blk_a = jnp.where(pairA == 0, z, lax.rem(z + nz - pairA, nz))
        blk_b = jnp.where(pairA == 0, lax.rem(z + half, nz), lax.rem(z + pairA, nz))
        tl = (nA * TILE + lax.broadcasted_iota(jnp.int32, (NEW_PAD, TILE), 1)) // ratio
        qtok = jnp.where(tl < 2 * tok, 2 * tok * blk_a + tl, 2 * tok * blk_b + tl - 2 * tok)
        kid = lax.broadcasted_iota(jnp.int32, (NEW_PAD, TILE), 0)
        pn = []
        for q in (0, 1):
            pe = jnp.exp2(SN[1 - par][q] * csc - mc)
            l = l + colsum(pe)
            pn += [pe.astype(BF16), jnp.zeros((128 - NEW_PAD, TILE), BF16)]
            ktok = 2 * tok * z + tok * q + kid
            sv = jnp.where((kid < tok) & (ktok <= qtok), dot(knbuf[q, hA], QT[par][0:hd, :]), NEG)
            SN[par][q] = sv
            mm = jnp.maximum(mm, colmax(sv))
        acc = acc + dot(jnp.concatenate([vnbuf[0, hB], vnbuf[1, hB]], axis=1), jnp.concatenate(pn, axis=0))
        lt = jnp.sum(l, axis=0, keepdims=True)
        sl = pl.ds(pl.multiple_of(nB * TILE, TILE), TILE)
        plse[hB, pairB, :, sl] = m * scale + jnp.log(lt)
        po[hB, pairB, :, sl] = (acc * (1.0 / lt)).astype(BF16)
        return mm

    for f, a in ev[0]:
        f(*a)
    kv_wait(0)
    for there, here in new_in():
        here.wait()
        there.wait_recv()
    make_qt(0, 0)

    def pair_of_tiles(t, mm):
        for i in range(1, bodies):
            if ev[i]:
                @pl.when(t == i)
                def _(i=i):
                    for f, a in ev[i]:
                        f(*a)
        return tile(2 * t, tile(2 * t - 1, mm, 0), 1)

    lax.fori_loop(0, bodies, pair_of_tiles, jnp.zeros((8, TILE), F32))

    for f, a in ev[bodies]:
        f(*a)
    fin = (remote(lseb, lse_hbm.at[c], fin_sem.at[0], fin_sem.at[1], partner),
           pltpu.make_async_copy(lseb, lse_hbm.at[c], fin_sem.at[2]))
    for cp in fin:
        cp.start()

    for h in range(heads):
        q_in(h)[0].wait_send()
        for there in kv_in(h):
            there.wait_send()
        for d in (0, 1):
            for k in range(half):
                if k + 1 < half or far_dir(h) == d:
                    ag(h, d, k).wait_send()
            for k in range(1, half + 1):
                if k < half or far_dir(h) == d:
                    for cp in rs(h, d, k):
                        cp.wait_send()
        there, here = out_copies(h)
        here.wait()
        there.wait()
    for there, _ in new_in():
        there.wait_send()
    fin[1].wait()
    fin[0].wait()


def solution(mesh):
    nz = mesh.shape["cp"] // 2
    tok_spec = P(("dp", "cp"))

    def local(queries, key_new, value_new, key_cache, value_cache, prefix_len):
        tok, nq, hd = queries.shape
        cache, nkv = key_cache.shape[0], key_cache.shape[1]
        ratio = nq // nkv
        heads = nkv // 2
        half = nz // 2
        rank = lax.axis_index("cp")
        c = rank % 2
        kn = jnp.pad(key_new.transpose(1, 0, 2), ((0, 0), (0, NEW_PAD - tok), (0, 0)))
        vn = jnp.pad(value_new.transpose(1, 2, 0), ((0, 0), (0, 0), (0, 128 - tok)))
        rows, keys = 2 * tok * ratio, 2 * cache
        dma = pltpu.SemaphoreType.DMA
        out, lse = pl.pallas_call(
            functools.partial(_attend, nz, tok, heads, ratio, cache),
            out_shape=(jax.ShapeDtypeStruct((tok, nq, hd), BF16), jax.ShapeDtypeStruct((2, 8, rows), F32)),
            in_specs=[pl.BlockSpec(memory_space=pl.ANY)] * 5 + [pl.BlockSpec(memory_space=pltpu.SMEM)],
            out_specs=[pl.BlockSpec(memory_space=pl.ANY)] * 2,
            scratch_shapes=[
                pltpu.VMEM((heads, keys, hd), BF16), pltpu.VMEM((heads, hd, keys), BF16),
                pltpu.VMEM((2, heads, NEW_PAD, hd), BF16), pltpu.VMEM((2, heads, hd, 128), BF16),
                pltpu.VMEM((heads, half, 4 * tok, ratio, hd), BF16),
                pltpu.VMEM((keys, TILE), F32), pltpu.VMEM((keys, TILE), F32),
                pltpu.VMEM((2, NEW_PAD, TILE), F32), pltpu.VMEM((2, NEW_PAD, TILE), F32),
                pltpu.VMEM((keys, hd), BF16),
                pltpu.VMEM((TILE, TILE), BF16), pltpu.VMEM((TILE, TILE), BF16),
                pltpu.VMEM((heads, half, hd, 2 * rows), BF16), pltpu.VMEM((heads, half, 1, 2 * rows), F32),
                pltpu.VMEM((2, heads, half, hd, rows), BF16), pltpu.VMEM((2, heads, half, 1, rows), F32),
                pltpu.VMEM((heads, 2 * tok, ratio, hd), BF16), pltpu.VMEM((8, rows), F32),
                pltpu.VMEM((cache * nkv, hd), BF16), pltpu.VMEM((cache * nkv, hd), BF16), pltpu.VMEM((CHUNK * nkv, hd), F32),
                pltpu.VMEM((heads, cache, hd), BF16), pltpu.VMEM((heads, hd, cache), BF16),
                dma((2,)), dma((2, heads)), dma((2, heads)), dma((2, 3)),
                dma((heads,)), dma((heads,)), dma((heads,)),
                dma((2, heads, half)), dma((2, heads, half)),
                dma((2, heads, half)), dma((2, heads, half)),
                dma((2, heads, half)), dma((2, heads, half)),
                dma((heads, 3)), dma((3,)),
            ],
            compiler_params=pltpu.CompilerParams(collective_id=0, has_side_effects=True, vmem_limit_bytes=60 * 2**20),
            name="ring_attend",
        )(queries, key_cache.reshape(cache * nkv, hd), value_cache.reshape(cache * nkv, hd), kn, vn, prefix_len)
        lse = lse[:, :heads].reshape(nkv, 2, tok, ratio)
        lse = lax.dynamic_index_in_dim(lse, c, axis=1, keepdims=False)
        row_lse = lse.transpose(1, 0, 2).reshape(tok, nq)
        return out, row_lse

    return jax.shard_map(local, mesh=mesh, in_specs=(tok_spec,) * 5 + (P("dp"),), out_specs=(tok_spec, tok_spec), check_vma=False)
```

```python
import functools

import jax
import jax.numpy as jnp
from jax import lax
from jax.experimental import pallas as pl
from jax.experimental.pallas import tpu as pltpu
from jax.sharding import PartitionSpec as P

NEG = -1e30
LOG2E = 1.4426950408889634
F32 = jnp.float32
BF16 = jnp.bfloat16
TILE = 256
NEW_PAD = 32
SUB = 2048
CHUNK = 256


def _attend(nz, tok, heads, ratio, cache,
            q_hbm, k_hbm, v_hbm, kn_hbm, vn_hbm, plen_ref, out_hbm, lse_hbm,
            kbuf, vbuf, knbuf, vnbuf, qbuf, s0, s1, sn0, sn1, bias, qt0, qt1,
            po, plse, rb, rl, outb, lseb, rawk, rawv, st, ksend, vsend, rawn, knsend, vnsend,
            raw_sem, kv_send, kv_recv, kn_sem, q_loc, q_send, q_recv,
            ag_send, ag_recv, ro_send, ro_recv, rs_send, rs_recv, out_sem, fin_sem):
    hd = q_hbm.shape[-1]
    scale = hd ** -0.5
    csc = scale * LOG2E
    half = nz // 2
    rows = 2 * tok * ratio
    mine = tok * ratio
    keys = 2 * cache
    per_step = 2 * rows // TILE
    steps = heads * half
    tiles = steps * per_step
    bodies = tiles // 2

    rank = lax.axis_index("cp")
    z, c = rank // 2, rank % 2
    partner = 2 * z + (1 - c)
    right = 2 * lax.rem(z + 1, nz) + c
    left = 2 * lax.rem(z + nz - 1, nz) + c
    to = (right, left)

    barrier = pltpu.get_barrier_semaphore()
    for dev in (partner, right, left):
        pl.semaphore_signal(barrier, inc=1, device_id={"cp": dev}, device_id_type=pl.DeviceIdType.MESH)
    pl.semaphore_wait(barrier, 3)

    def remote(src, dst, ss, rs, dev):
        return pltpu.make_async_remote_copy(src_ref=src, dst_ref=dst, send_sem=ss, recv_sem=rs,
                                            device_id={"cp": dev}, device_id_type=pl.DeviceIdType.MESH)

    def head_rows(ref, n):
        return ref.at[:, pl.ds(pl.multiple_of(n * ratio, ratio), ratio), :]

    def q_in(h):
        dst = qbuf.at[h, 0, pl.ds(c * tok, tok)]
        there = remote(head_rows(q_hbm, heads * (1 - c) + h), dst, q_send.at[h], q_recv.at[h], partner)
        here = pltpu.make_async_copy(head_rows(q_hbm, heads * c + h), dst, q_loc.at[h])
        return there, here

    def raw_in():
        return [pltpu.make_async_copy(src, dst, raw_sem.at[n]) for n, (src, dst) in enumerate(((k_hbm, rawk), (v_hbm, rawv)))]

    def kv_in(h):
        return [remote(ksend.at[h], kbuf.at[h, pl.ds(c * cache, cache), :], kv_send.at[0, h], kv_recv.at[0, h], partner),
                remote(vsend.at[h], vbuf.at[h, :, pl.ds(c * cache, cache)], kv_send.at[1, h], kv_recv.at[1, h], partner)]

    def relayout(raw, put):
        def chunk(i, _):
            st[...] = raw[pl.ds(pl.multiple_of(i * CHUNK * 2 * heads, CHUNK * 2 * heads), CHUNK * 2 * heads), :].astype(F32)
            ok = rank * cache + i * CHUNK + lax.broadcasted_iota(jnp.int32, (CHUNK, hd), 0) < plen_ref[0]
            at0 = pl.multiple_of(i * CHUNK, CHUNK)
            for h in range(heads):
                for own, n in ((True, heads * c + h), (False, heads * (1 - c) + h)):
                    put(own, h, at0, jnp.where(ok, st[pl.ds(n, CHUNK, stride=2 * heads), :], 0.0))
            return 0
        lax.fori_loop(0, cache // CHUNK, chunk, 0)

    def put_k(own, h, at0, x):
        if own:
            kbuf[h, pl.ds(pl.multiple_of(c * cache + at0, CHUNK), CHUNK), :] = x.astype(BF16)
        else:
            ksend[h, pl.ds(at0, CHUNK), :] = x.astype(BF16)

    def put_v(own, h, at0, x):
        if own:
            vbuf[h, :, pl.ds(pl.multiple_of(c * cache + at0, CHUNK), CHUNK)] = x.T.astype(BF16)
        else:
            vsend[h, :, pl.ds(at0, CHUNK)] = x.T.astype(BF16)

    def new_raw():
        return [pltpu.make_async_copy(src, rawn.at[n], kn_sem.at[n, 2]) for n, src in enumerate((kn_hbm, vn_hbm))]

    def new_in():
        return [remote(src, dst.at[c], kn_sem.at[n, 0], kn_sem.at[n, 1], partner)
                for n, (src, dst) in enumerate(((knsend, knbuf), (vnsend, vnbuf)))]

    def relayout_new():
        for n, (pad, mine, theirs) in enumerate(((NEW_PAD, knbuf, knsend), (hd, vnbuf, vnsend))):
            st[0:tok * 2 * heads, :] = rawn[n].astype(F32)
            for h in range(heads):
                for own, src in ((True, heads * c + h), (False, heads * (1 - c) + h)):
                    x = st[pl.ds(src, tok, stride=2 * heads), :]
                    x = jnp.concatenate([x, jnp.zeros((pad - tok, hd), F32)], axis=0)
                    x = (x if n == 0 else x.T).astype(BF16)
                    if own:
                        mine[c, h] = x
                    else:
                        theirs[h] = x

    def q_slot(h, d, k):
        if k == 0:
            return qbuf.at[h, 0, pl.ds(0, 2 * tok)]
        if k == half:
            return qbuf.at[h, 0, pl.ds(2 * tok, 2 * tok)]
        return qbuf.at[h, k, pl.ds(d * 2 * tok, 2 * tok)]

    def far_dir(h):
        return h % 2

    def ag(h, d, k):
        return remote(q_slot(h, d, k), q_slot(h, d, k + 1), ag_send.at[d, h, k], ag_recv.at[d, h, k], to[d])

    def ag_start(h, k):
        for d in (0, 1):
            if k + 1 < half or far_dir(h) == d:
                ag(h, d, k).start()

    def ag_wait(h, k):
        for d in (0, 1):
            if k + 1 < half or far_dir(h) == d:
                ag(h, d, k).wait_recv()

    def hop(h, k):
        ag_wait(h, k)
        if k + 1 < half:
            ag_start(h, k + 1)

    def po_part(h, d, k):
        if k == half:
            sl = pl.ds(rows, rows)
            return po.at[h, 0, :, sl], plse.at[h, 0, :, sl]
        sl = pl.ds((1 - d) * rows, rows)
        return po.at[h, k, :, sl], plse.at[h, k, :, sl]

    def rs(h, d, k):
        o, l = po_part(h, d, k)
        return (remote(o, rb.at[d, h, k - 1], ro_send.at[d, h, k - 1], ro_recv.at[d, h, k - 1], to[d]),
                remote(l, rl.at[d, h, k - 1], rs_send.at[d, h, k - 1], rs_recv.at[d, h, k - 1], to[d]))

    def merge(parts):
        top = functools.reduce(jnp.maximum, [l for _, l in parts])
        ws = [jnp.exp(l - top) for _, l in parts]
        tot = functools.reduce(jnp.add, ws)
        inv = 1.0 / tot
        acc = functools.reduce(jnp.add, [o.astype(F32) * (w * inv) for (o, _), w in zip(parts, ws)])
        return acc, top + jnp.log(tot)

    def rs_stage(h, k):
        for d in (0, 1):
            if k == half and far_dir(h) != d:
                continue
            if k + 1 < half or (k + 1 == half and far_dir(h) == d):
                for cp in rs(h, d, k + 1):
                    cp.wait_recv()
                o, l = po_part(h, d, k)
                acc, lse = merge([(o[...], l[...]), (rb[d, h, k], rl[d, h, k])])
                o[...] = acc.astype(BF16)
                l[...] = lse
            for cp in rs(h, d, k):
                cp.start()

    def out_copies(h):
        dst = head_rows(out_hbm, heads * c + h)
        there = remote(outb.at[h, pl.ds((1 - c) * tok, tok)], dst, out_sem.at[h, 0], out_sem.at[h, 1], partner)
        here = pltpu.make_async_copy(outb.at[h, pl.ds(c * tok, tok)], dst, out_sem.at[h, 2])
        return there, here

    def final(h):
        for d in (0, 1):
            for cp in rs(h, d, 1):
                cp.wait_recv()
        acc, lse = merge([(po[h, 0, :, 0:rows], plse[h, 0, :, 0:rows])] + [(rb[d, h, 0], rl[d, h, 0]) for d in (0, 1)])
        outb[h] = acc.T.reshape(2 * tok, ratio, hd).astype(BF16)
        lseb[h:h + 1, :] = lse
        for cp in out_copies(h):
            cp.start()

    def kv_wait(h):
        for there in kv_in(h):
            there.wait_recv()

    for h in range(heads):
        for cp in q_in(h):
            cp.start()
    for cp in raw_in():
        cp.start()
    for cp in new_raw():
        cp.start()

    def q_wait_send(h):
        there, here = q_in(h)
        here.wait()
        there.wait_recv()
        ag_start(h, 0)

    pos = z * keys + lax.broadcasted_iota(jnp.int32, (keys, hd), 0)
    lane = lax.broadcasted_iota(jnp.int32, (keys, hd), 1)
    bias[...] = jnp.where((pos >= plen_ref[0]) & (lane == 0), NEG, 0.0).astype(BF16)
    ones = jnp.where(lax.broadcasted_iota(jnp.int32, (TILE - hd, TILE), 0) == 0, 1.0, 0.0).astype(BF16)
    for r in (qt0, qt1):
        r[hd:TILE, :] = ones
    lseb[...] = jnp.zeros_like(lseb)
    QT, SR, SN = (qt0, qt1), (s0, s1), (sn0, sn1)

    for h in (0, 1):
        q_wait_send(h)
    for cp in new_raw():
        cp.wait()
    relayout_new()
    for cp in new_in():
        cp.start()
    raw_in()[0].wait()
    relayout(rawk, put_k)
    for h in range(heads):
        kv_in(h)[0].start()
    hop(0, 0)
    raw_in()[1].wait()
    relayout(rawv, put_v)
    for h in range(heads):
        kv_in(h)[1].start()

    ev = {i: [] for i in range(bodies + 1)}

    def at(i, f, *a):
        ev[min(i, bodies)].append((f, a))

    table = {
        0: [(q_wait_send, 3), (hop, 1, 0)], 1: [(q_wait_send, 2)], 2: [(hop, 0, 1)], 3: [(hop, 1, 1)],
        4: [(hop, 0, 2), (hop, 2, 0), (hop, 3, 0)], 6: [(hop, 0, 3), (hop, 1, 2)], 7: [(hop, 2, 1)], 8: [(hop, 3, 1)],
        9: [(hop, 1, 3), (hop, 2, 2)], 11: [(rs_stage, 0, 4), (hop, 2, 3)], 12: [(hop, 3, 2), (rs_stage, 1, 4)],
        14: [(rs_stage, 2, 4), (rs_stage, 0, 3)], 15: [(rs_stage, 1, 3)], 16: [(rs_stage, 2, 3), (hop, 3, 3)],
        18: [(rs_stage, 0, 2)], 19: [(rs_stage, 2, 2)], 20: [(rs_stage, 3, 4), (rs_stage, 1, 2)],
        21: [(rs_stage, 2, 1), (rs_stage, 3, 3)], 22: [(rs_stage, 0, 1)], 23: [(rs_stage, 3, 2), (rs_stage, 1, 1), (final, 2)],
        24: [(rs_stage, 3, 1), (final, 0), (final, 1), (final, 3)],
    }
    for i, fs in table.items():
        for f, *a in fs:
            at(i, f, *a)
    at(0, kv_wait, 1)
    at(11, kv_wait, 2)
    at(17, kv_wait, 3)

    def place(t):
        s, n = t // per_step, lax.rem(t, per_step)
        early = s < 2 * half
        h = jnp.where(early, lax.rem(s, 2), s // half)
        pair = jnp.where(early, lax.rem(s // 2 + 1, half), lax.rem(2 * half - lax.rem(s, half), half))
        return h, pair, n

    def make_qt(t, slot):
        h, pair, n = place(jnp.clip(t, 0, tiles - 1))
        q = qbuf[h, pair, pl.ds(n * (TILE // ratio), TILE // ratio)].astype(F32).reshape(TILE, hd)
        QT[slot][0:hd, :] = q.T.astype(BF16)

    def dot(a, b):
        return lax.dot_general(a, b, (((1,), (0,)), ((), ())), preferred_element_type=F32)

    def colmax(x):
        return jnp.max(x.reshape(x.shape[0] // 8, 8, TILE), axis=0)

    def colsum(x):
        return jnp.sum(x.reshape(x.shape[0] // 8, 8, TILE), axis=0)

    def scores(t, par, mm, u):
        h, pair, n = place(jnp.clip(t, 0, tiles - 1))
        sl = pl.ds(u * SUB, SUB)
        lhs = jnp.concatenate([kbuf[h, sl, :], bias[sl, :]], axis=1)
        if u == 0:
            kn = jnp.concatenate([knbuf[0, h], knbuf[1, h]], axis=0)
            lhs = jnp.concatenate([lhs, jnp.concatenate([kn, jnp.zeros((2 * NEW_PAD, TILE - hd), BF16)], axis=1)], axis=0)
        sv = dot(lhs, QT[par][...])
        if u == 0:
            blk_a = jnp.where(pair == 0, z, lax.rem(z + nz - pair, nz))
            blk_b = jnp.where(pair == 0, lax.rem(z + half, nz), lax.rem(z + pair, nz))
            tl = lax.shift_right_logical(n * TILE + lax.broadcasted_iota(jnp.int32, (NEW_PAD, TILE), 1), ratio.bit_length() - 1)
            last = jnp.where(tl < 2 * tok, 2 * tok * (blk_a - z) + tl, 2 * tok * (blk_b - z - 1) + tl)
            kid = lax.broadcasted_iota(jnp.int32, (NEW_PAD, TILE), 0)
            for q in (0, 1):
                x = jnp.where((kid < tok) & (kid + tok * q <= last), sv[SUB + q * NEW_PAD:SUB + (q + 1) * NEW_PAD], NEG)
                SN[par][q] = x
                mm = jnp.maximum(mm, colmax(x))
            sv = sv[:SUB]
        SR[par][sl, :] = sv
        return jnp.maximum(mm, colmax(sv))

    def tile(i, mm, par):
        h, pair, n = place(i)
        m = jnp.max(mm, axis=0, keepdims=True)
        mc = m * csc
        mm = jnp.full((8, TILE), -jnp.inf, F32)
        l = jnp.zeros((8, TILE), F32)
        pn = []
        for q in (0, 1):
            pe = jnp.exp2(SN[1 - par][q] * csc - mc)
            l = l + colsum(pe)
            pn += [pe.astype(BF16), jnp.zeros((128 - NEW_PAD, TILE), BF16)]
        acc = dot(jnp.concatenate([vnbuf[0, h], vnbuf[1, h]], axis=1), jnp.concatenate(pn, axis=0))
        for u in range(keys // SUB):
            sl = pl.ds(u * SUB, SUB)
            mm = scores(i + 1, par, mm, u)
            if u == 0:
                make_qt(i + 2, 1 - par)
            pe = jnp.exp2(SR[1 - par][sl, :] * csc - mc)
            l = l + colsum(pe)
            acc = acc + dot(vbuf[h, :, sl], pe.astype(BF16))
        lt = jnp.sum(l, axis=0, keepdims=True)
        sl = pl.ds(pl.multiple_of(n * TILE, TILE), TILE)
        plse[h, pair, :, sl] = m * scale + jnp.log(lt)
        po[h, pair, :, sl] = (acc * (1.0 / lt)).astype(BF16)
        return mm

    kv_wait(0)
    for cp in new_in():
        cp.wait_recv()
    make_qt(0, 0)
    first = jnp.full((8, TILE), -jnp.inf, F32)
    for u in range(keys // SUB):
        first = scores(0, 0, first, u)
    make_qt(1, 1)
    for f, a in ev[0]:
        f(*a)

    def pair_of_tiles(t, mm):
        for i in range(1, bodies):
            if ev[i]:
                @pl.when(t == i)
                def _(i=i):
                    for f, a in ev[i]:
                        f(*a)
        return tile(2 * t + 1, tile(2 * t, mm, 1), 0)

    lax.fori_loop(0, bodies, pair_of_tiles, first)

    for f, a in ev[bodies]:
        f(*a)
    fin = (remote(lseb, lse_hbm.at[c], fin_sem.at[0], fin_sem.at[1], partner),
           pltpu.make_async_copy(lseb, lse_hbm.at[c], fin_sem.at[2]))
    for cp in fin:
        cp.start()

    for h in range(heads):
        q_in(h)[0].wait_send()
        for there in kv_in(h):
            there.wait_send()
        for d in (0, 1):
            for k in range(half):
                if k + 1 < half or far_dir(h) == d:
                    ag(h, d, k).wait_send()
            for k in range(1, half + 1):
                if k < half or far_dir(h) == d:
                    for cp in rs(h, d, k):
                        cp.wait_send()
        there, here = out_copies(h)
        here.wait()
        there.wait()
    for cp in new_in():
        cp.wait_send()
    fin[1].wait()
    fin[0].wait()


def solution(mesh):
    nz = mesh.shape["cp"] // 2
    tok_spec = P(("dp", "cp"))

    def local(queries, key_new, value_new, key_cache, value_cache, prefix_len):
        tok, nq, hd = queries.shape
        cache, nkv = key_cache.shape[0], key_cache.shape[1]
        ratio = nq // nkv
        heads = nkv // 2
        half = nz // 2
        rank = lax.axis_index("cp")
        c = rank % 2
        rows, keys = 2 * tok * ratio, 2 * cache
        dma = pltpu.SemaphoreType.DMA
        out, lse = pl.pallas_call(
            functools.partial(_attend, nz, tok, heads, ratio, cache),
            out_shape=(jax.ShapeDtypeStruct((tok, nq, hd), BF16), jax.ShapeDtypeStruct((2, 8, rows), F32)),
            in_specs=[pl.BlockSpec(memory_space=pl.ANY)] * 5 + [pl.BlockSpec(memory_space=pltpu.SMEM)],
            out_specs=[pl.BlockSpec(memory_space=pl.ANY)] * 2,
            scratch_shapes=[
                pltpu.VMEM((heads, keys, hd), BF16), pltpu.VMEM((heads, hd, keys), BF16),
                pltpu.VMEM((2, heads, NEW_PAD, hd), BF16), pltpu.VMEM((2, heads, hd, hd), BF16),
                pltpu.VMEM((heads, half, 4 * tok, ratio, hd), BF16),
                pltpu.VMEM((keys, TILE), F32), pltpu.VMEM((keys, TILE), F32),
                pltpu.VMEM((2, NEW_PAD, TILE), F32), pltpu.VMEM((2, NEW_PAD, TILE), F32),
                pltpu.VMEM((keys, hd), BF16),
                pltpu.VMEM((TILE, TILE), BF16), pltpu.VMEM((TILE, TILE), BF16),
                pltpu.VMEM((heads, half, hd, 2 * rows), BF16), pltpu.VMEM((heads, half, 1, 2 * rows), F32),
                pltpu.VMEM((2, heads, half, hd, rows), BF16), pltpu.VMEM((2, heads, half, 1, rows), F32),
                pltpu.VMEM((heads, 2 * tok, ratio, hd), BF16), pltpu.VMEM((8, rows), F32),
                pltpu.VMEM((cache * nkv, hd), BF16), pltpu.VMEM((cache * nkv, hd), BF16), pltpu.VMEM((CHUNK * nkv, hd), F32),
                pltpu.VMEM((heads, cache, hd), BF16), pltpu.VMEM((heads, hd, cache), BF16),
                pltpu.VMEM((2, tok * nkv, hd), BF16), pltpu.VMEM((heads, NEW_PAD, hd), BF16), pltpu.VMEM((heads, hd, hd), BF16),
                dma((2,)), dma((2, heads)), dma((2, heads)), dma((2, 3)),
                dma((heads,)), dma((heads,)), dma((heads,)),
                dma((2, heads, half)), dma((2, heads, half)),
                dma((2, heads, half)), dma((2, heads, half)),
                dma((2, heads, half)), dma((2, heads, half)),
                dma((heads, 3)), dma((3,)),
            ],
            compiler_params=pltpu.CompilerParams(collective_id=0, has_side_effects=True, vmem_limit_bytes=60 * 2**20),
            name="ring_attend",
        )(queries, key_cache.reshape(cache * nkv, hd), value_cache.reshape(cache * nkv, hd),
          key_new.reshape(tok * nkv, hd), value_new.reshape(tok * nkv, hd), prefix_len)
        lse = lse[:, :heads].reshape(nkv, 2, tok, ratio)
        lse = lax.dynamic_index_in_dim(lse, c, axis=1, keepdims=False)
        row_lse = lse.transpose(1, 0, 2).reshape(tok, nq)
        return out, row_lse

    return jax.shard_map(local, mesh=mesh, in_specs=(tok_spec,) * 5 + (P("dp"),), out_specs=(tok_spec, tok_spec), check_vma=False)
```

```python
import functools

import jax
import jax.numpy as jnp
from jax import lax
from jax.experimental import pallas as pl
from jax.experimental.pallas import tpu as pltpu
from jax.sharding import PartitionSpec as P

NEG = -1e30
LOG2E = 1.4426950408889634
F32 = jnp.float32
BF16 = jnp.bfloat16
TILE = 256
NEW_PAD = 32
SUB = 4096
CHUNK = 128


def _attend(nz, tok, heads, ratio, cache,
            q_hbm, k_hbm, v_hbm, kn_hbm, vn_hbm, plen_ref, out_hbm, lse_hbm,
            kbuf, vbuf, knbuf, vnbuf, qbuf, s0, s1, sn0, sn1, bias, qt0, qt1,
            po, plse, rb, rl, outb, lseb, rawk, rawv, st0, st1, ksend, vsend, rawn, knsend, vnsend,
            raw_sem, kv_send, kv_recv, kn_sem, q_loc, q_send, q_recv,
            ag_send, ag_recv, ro_send, ro_recv, rs_send, rs_recv, out_sem, fin_sem):
    hd = q_hbm.shape[-1]
    scale = hd ** -0.5
    csc = scale * LOG2E
    half = nz // 2
    rows = 2 * tok * ratio
    mine = tok * ratio
    keys = 2 * cache
    per_step = 2 * rows // TILE
    steps = heads * half
    tiles = steps * per_step
    bodies = tiles // 2

    rank = lax.axis_index("cp")
    z, c = rank // 2, rank % 2
    partner = 2 * z + (1 - c)
    right = 2 * lax.rem(z + 1, nz) + c
    left = 2 * lax.rem(z + nz - 1, nz) + c
    to = (right, left)

    barrier = pltpu.get_barrier_semaphore()
    for dev in (partner, right, left):
        pl.semaphore_signal(barrier, inc=1, device_id={"cp": dev}, device_id_type=pl.DeviceIdType.MESH)
    pl.semaphore_wait(barrier, 3)

    def remote(src, dst, ss, rs, dev):
        return pltpu.make_async_remote_copy(src_ref=src, dst_ref=dst, send_sem=ss, recv_sem=rs,
                                            device_id={"cp": dev}, device_id_type=pl.DeviceIdType.MESH)

    def head_rows(ref, n):
        return ref.at[:, pl.ds(pl.multiple_of(n * ratio, ratio), ratio), :]

    def q_in(h):
        dst = qbuf.at[h, 0, pl.ds(c * tok, tok)]
        there = remote(head_rows(q_hbm, heads * (1 - c) + h), dst, q_send.at[h], q_recv.at[h], partner)
        here = pltpu.make_async_copy(head_rows(q_hbm, heads * c + h), dst, q_loc.at[h])
        return there, here

    def raw_in():
        return [pltpu.make_async_copy(src, dst, raw_sem.at[n]) for n, (src, dst) in enumerate(((k_hbm, rawk), (v_hbm, rawv)))]

    def kv_in(h):
        return [remote(ksend.at[h], kbuf.at[h, pl.ds(c * cache, cache), :], kv_send.at[0, h], kv_recv.at[0, h], partner),
                remote(vsend.at[h], vbuf.at[h, :, pl.ds(c * cache, cache)], kv_send.at[1, h], kv_recv.at[1, h], partner)]

    def relayout(raw, put):
        def chunk(i, st):
            st[...] = raw[pl.ds(pl.multiple_of(i * CHUNK * 2 * heads, CHUNK * 2 * heads), CHUNK * 2 * heads), :].astype(F32)
            ok = rank * cache + i * CHUNK + lax.broadcasted_iota(jnp.int32, (CHUNK, hd), 0) < plen_ref[0]
            at0 = pl.multiple_of(i * CHUNK, CHUNK)
            for h in range(heads):
                for own, n in ((True, heads * c + h), (False, heads * (1 - c) + h)):
                    put(own, h, at0, jnp.where(ok, st[pl.ds(n, CHUNK, stride=2 * heads), :], 0.0))

        def two(i, _):
            chunk(2 * i, st0)
            chunk(2 * i + 1, st1)
            return 0
        lax.fori_loop(0, cache // (2 * CHUNK), two, 0)

    def put_k(own, h, at0, x):
        if own:
            kbuf[h, pl.ds(pl.multiple_of(c * cache + at0, CHUNK), CHUNK), :] = x.astype(BF16)
        else:
            ksend[h, pl.ds(at0, CHUNK), :] = x.astype(BF16)

    def put_v(own, h, at0, x):
        if own:
            vbuf[h, :, pl.ds(pl.multiple_of(c * cache + at0, CHUNK), CHUNK)] = x.T.astype(BF16)
        else:
            vsend[h, :, pl.ds(at0, CHUNK)] = x.T.astype(BF16)

    def new_raw():
        return [pltpu.make_async_copy(src, rawn.at[n], kn_sem.at[n, 2]) for n, src in enumerate((kn_hbm, vn_hbm))]

    def new_in():
        return [remote(src, dst.at[c], kn_sem.at[n, 0], kn_sem.at[n, 1], partner)
                for n, (src, dst) in enumerate(((knsend, knbuf), (vnsend, vnbuf)))]

    def relayout_new():
        for n, (pad, mine, theirs) in enumerate(((NEW_PAD, knbuf, knsend), (hd, vnbuf, vnsend))):
            st0[0:tok * 2 * heads, :] = rawn[n].astype(F32)
            for h in range(heads):
                for own, src in ((True, heads * c + h), (False, heads * (1 - c) + h)):
                    x = st0[pl.ds(src, tok, stride=2 * heads), :]
                    x = jnp.concatenate([x, jnp.zeros((pad - tok, hd), F32)], axis=0)
                    x = (x if n == 0 else x.T).astype(BF16)
                    if own:
                        mine[c, h] = x
                    else:
                        theirs[h] = x

    def q_slot(h, d, k):
        if k == 0:
            return qbuf.at[h, 0, pl.ds(0, 2 * tok)]
        if k == half:
            return qbuf.at[h, 0, pl.ds(2 * tok, 2 * tok)]
        return qbuf.at[h, k, pl.ds(d * 2 * tok, 2 * tok)]

    def far_dir(h):
        return h % 2

    def ag(h, d, k):
        return remote(q_slot(h, d, k), q_slot(h, d, k + 1), ag_send.at[d, h, k], ag_recv.at[d, h, k], to[d])

    def ag_start(h, k):
        for d in (0, 1):
            if k + 1 < half or far_dir(h) == d:
                ag(h, d, k).start()

    def ag_wait(h, k):
        for d in (0, 1):
            if k + 1 < half or far_dir(h) == d:
                ag(h, d, k).wait_recv()

    def hop(h, k):
        ag_wait(h, k)
        if k + 1 < half:
            ag_start(h, k + 1)

    def po_part(h, d, k):
        if k == half:
            sl = pl.ds(rows, rows)
            return po.at[h, 0, :, sl], plse.at[h, 0, :, sl]
        sl = pl.ds((1 - d) * rows, rows)
        return po.at[h, k, :, sl], plse.at[h, k, :, sl]

    def rs(h, d, k):
        o, l = po_part(h, d, k)
        return (remote(o, rb.at[d, h, k - 1], ro_send.at[d, h, k - 1], ro_recv.at[d, h, k - 1], to[d]),
                remote(l, rl.at[d, h, k - 1], rs_send.at[d, h, k - 1], rs_recv.at[d, h, k - 1], to[d]))

    def merge(parts):
        top = functools.reduce(jnp.maximum, [l for _, l in parts])
        ws = [jnp.exp(l - top) for _, l in parts]
        tot = functools.reduce(jnp.add, ws)
        inv = 1.0 / tot
        acc = functools.reduce(jnp.add, [o.astype(F32) * (w * inv) for (o, _), w in zip(parts, ws)])
        return acc, top + jnp.log(tot)

    def rs_stage(h, k):
        for d in (0, 1):
            if k == half and far_dir(h) != d:
                continue
            if k + 1 < half or (k + 1 == half and far_dir(h) == d):
                for cp in rs(h, d, k + 1):
                    cp.wait_recv()
                o, l = po_part(h, d, k)
                acc, lse = merge([(o[...], l[...]), (rb[d, h, k], rl[d, h, k])])
                o[...] = acc.astype(BF16)
                l[...] = lse
            for cp in rs(h, d, k):
                cp.start()

    def out_copies(h):
        dst = head_rows(out_hbm, heads * c + h)
        there = remote(outb.at[h, pl.ds((1 - c) * tok, tok)], dst, out_sem.at[h, 0], out_sem.at[h, 1], partner)
        here = pltpu.make_async_copy(outb.at[h, pl.ds(c * tok, tok)], dst, out_sem.at[h, 2])
        return there, here

    def final(h):
        for d in (0, 1):
            for cp in rs(h, d, 1):
                cp.wait_recv()
        acc, lse = merge([(po[h, 0, :, 0:rows], plse[h, 0, :, 0:rows])] + [(rb[d, h, 0], rl[d, h, 0]) for d in (0, 1)])
        outb[h] = acc.T.reshape(2 * tok, ratio, hd).astype(BF16)
        lseb[h:h + 1, :] = lse
        for cp in out_copies(h):
            cp.start()

    def kv_wait(h):
        for there in kv_in(h):
            there.wait_recv()

    def kv_wait_one(h, n):
        kv_in(h)[n].wait_recv()

    for h in range(heads):
        for cp in q_in(h):
            cp.start()
    for cp in raw_in():
        cp.start()
    for cp in new_raw():
        cp.start()

    def q_wait_send(h):
        there, here = q_in(h)
        here.wait()
        there.wait_recv()
        ag_start(h, 0)

    pos = z * keys + lax.broadcasted_iota(jnp.int32, (keys, hd), 0)
    lane = lax.broadcasted_iota(jnp.int32, (keys, hd), 1)
    bias[...] = jnp.where((pos >= plen_ref[0]) & (lane == 0), NEG, 0.0).astype(BF16)
    ones = jnp.where(lax.broadcasted_iota(jnp.int32, (TILE - hd, TILE), 0) == 0, 1.0, 0.0).astype(BF16)
    for r in (qt0, qt1):
        r[hd:TILE, :] = ones
    lseb[...] = jnp.zeros_like(lseb)
    QT, SR, SN = (qt0, qt1), (s0, s1), (sn0, sn1)

    for h in (0, 1):
        q_wait_send(h)
    for cp in new_raw():
        cp.wait()
    relayout_new()
    for cp in new_in():
        cp.start()
    raw_in()[0].wait()
    relayout(rawk, put_k)
    for h in range(heads):
        kv_in(h)[0].start()
    hop(0, 0)
    raw_in()[1].wait()
    relayout(rawv, put_v)
    for h in range(heads):
        kv_in(h)[1].start()

    ev = {i: [] for i in range(bodies + 1)}

    def at(i, f, *a):
        ev[min(i, bodies)].append((f, a))

    table = {
        0: [(hop, 1, 0), (q_wait_send, 2)], 1: [(q_wait_send, 3)], 2: [(hop, 0, 1), (hop, 1, 1)],
        4: [(hop, 3, 0)], 5: [(hop, 2, 0), (hop, 0, 2)], 6: [(hop, 1, 2)], 7: [(hop, 2, 1)],
        8: [(hop, 0, 3), (hop, 1, 3), (hop, 3, 1)], 9: [(hop, 2, 2)], 10: [(hop, 3, 2)],
        11: [(hop, 2, 3), (rs_stage, 0, 4)], 12: [(hop, 3, 3), (rs_stage, 1, 4)], 13: [(rs_stage, 0, 3)],
        14: [(rs_stage, 1, 3), (rs_stage, 2, 4)], 15: [(rs_stage, 3, 4), (rs_stage, 0, 2)], 17: [(rs_stage, 2, 3)],
        18: [(rs_stage, 3, 3), (rs_stage, 0, 1), (rs_stage, 1, 2)], 20: [(rs_stage, 2, 2)], 21: [(rs_stage, 3, 2), (final, 0)],
        22: [(rs_stage, 1, 1)], 23: [(rs_stage, 2, 1)],
        24: [(rs_stage, 3, 1), (final, 1), (final, 2), (final, 3)],
    }
    for i, fs in table.items():
        for f, *a in fs:
            at(i, f, *a)
    at(0, kv_wait, 1)
    at(11, kv_wait, 2)
    at(11, kv_wait, 3)

    def place(t):
        s, n = t // per_step, lax.rem(t, per_step)
        g = s // (2 * half)
        h = 2 * g + lax.rem(s, 2)
        r = (s - 2 * half * g) // 2
        pair = jnp.where(g == 0, lax.rem(r + 1, half), lax.rem(half - r, half))
        return h, pair, n

    def make_qt(t, slot):
        h, pair, n = place(jnp.clip(t, 0, tiles - 1))
        q = qbuf[h, pair, pl.ds(n * (TILE // ratio), TILE // ratio)].astype(F32).reshape(TILE, hd)
        QT[slot][0:hd, :] = q.T.astype(BF16)

    def dot(a, b):
        return lax.dot_general(a, b, (((1,), (0,)), ((), ())), preferred_element_type=F32)

    def colmax(x):
        return jnp.max(x.reshape(x.shape[0] // 8, 8, TILE), axis=0)

    def colsum(x):
        return jnp.sum(x.reshape(x.shape[0] // 8, 8, TILE), axis=0)

    def scores(t, par, mm, u):
        h, pair, n = place(jnp.clip(t, 0, tiles - 1))
        sl = pl.ds(u * SUB, SUB)
        lhs = jnp.concatenate([kbuf[h, sl, :], bias[sl, :]], axis=1)
        if u == 0:
            kn = jnp.concatenate([knbuf[0, h], knbuf[1, h]], axis=0)
            lhs = jnp.concatenate([lhs, jnp.concatenate([kn, jnp.zeros((2 * NEW_PAD, TILE - hd), BF16)], axis=1)], axis=0)
        sv = dot(lhs, QT[par][...])
        if u == 0:
            blk_a = jnp.where(pair == 0, z, lax.rem(z + nz - pair, nz))
            blk_b = jnp.where(pair == 0, lax.rem(z + half, nz), lax.rem(z + pair, nz))
            tl = lax.shift_right_logical(n * TILE + lax.broadcasted_iota(jnp.int32, (NEW_PAD, TILE), 1), ratio.bit_length() - 1)
            last = jnp.where(tl < 2 * tok, 2 * tok * (blk_a - z) + tl, 2 * tok * (blk_b - z - 1) + tl)
            kid = lax.broadcasted_iota(jnp.int32, (NEW_PAD, TILE), 0)
            for q in (0, 1):
                x = jnp.where((kid < tok) & (kid + tok * q <= last), sv[SUB + q * NEW_PAD:SUB + (q + 1) * NEW_PAD], NEG)
                SN[par][q] = x
                mm = jnp.maximum(mm, colmax(x))
            sv = sv[:SUB]
        SR[par][sl, :] = sv
        return jnp.maximum(mm, colmax(sv))

    def tile(i, mm, par):
        h, pair, n = place(i)
        m = jnp.max(mm, axis=0, keepdims=True)
        mc = m * csc
        mm = jnp.full((8, TILE), -jnp.inf, F32)
        l = jnp.zeros((8, TILE), F32)
        pn = []
        for q in (0, 1):
            pe = jnp.exp2(SN[1 - par][q] * csc - mc)
            l = l + colsum(pe)
            pn += [pe.astype(BF16), jnp.zeros((128 - NEW_PAD, TILE), BF16)]
        acc = dot(jnp.concatenate([vnbuf[0, h], vnbuf[1, h]], axis=1), jnp.concatenate(pn, axis=0))
        for u in range(keys // SUB):
            sl = pl.ds(u * SUB, SUB)
            mm = scores(i + 1, par, mm, u)
            pe = jnp.exp2(SR[1 - par][sl, :] * csc - mc)
            l = l + colsum(pe)
            acc = acc + dot(vbuf[h, :, sl], pe.astype(BF16))
        make_qt(i + 2, 1 - par)
        lt = jnp.sum(l, axis=0, keepdims=True)
        sl = pl.ds(pl.multiple_of(n * TILE, TILE), TILE)
        plse[h, pair, :, sl] = m * scale + jnp.log(lt)
        po[h, pair, :, sl] = (acc * (1.0 / lt)).astype(BF16)
        return mm

    kv_wait_one(0, 0)
    for cp in new_in():
        cp.wait_recv()
    make_qt(0, 0)
    first = jnp.full((8, TILE), -jnp.inf, F32)
    for u in range(keys // SUB):
        first = scores(0, 0, first, u)
    make_qt(1, 1)
    kv_wait_one(0, 1)
    for f, a in ev[0]:
        f(*a)

    def pair_of_tiles(t, mm):
        for i in range(1, bodies):
            if ev[i]:
                @pl.when(t == i)
                def _(i=i):
                    for f, a in ev[i]:
                        f(*a)
        return tile(2 * t + 1, tile(2 * t, mm, 1), 0)

    lax.fori_loop(0, bodies, pair_of_tiles, first)

    for f, a in ev[bodies]:
        f(*a)
    fin = (remote(lseb, lse_hbm.at[c], fin_sem.at[0], fin_sem.at[1], partner),
           pltpu.make_async_copy(lseb, lse_hbm.at[c], fin_sem.at[2]))
    for cp in fin:
        cp.start()

    for h in range(heads):
        q_in(h)[0].wait_send()
        for there in kv_in(h):
            there.wait_send()
        for d in (0, 1):
            for k in range(half):
                if k + 1 < half or far_dir(h) == d:
                    ag(h, d, k).wait_send()
            for k in range(1, half + 1):
                if k < half or far_dir(h) == d:
                    for cp in rs(h, d, k):
                        cp.wait_send()
        there, here = out_copies(h)
        here.wait()
        there.wait()
    for cp in new_in():
        cp.wait_send()
    fin[1].wait()
    fin[0].wait()


def solution(mesh):
    nz = mesh.shape["cp"] // 2
    tok_spec = P(("dp", "cp"))

    def local(queries, key_new, value_new, key_cache, value_cache, prefix_len):
        tok, nq, hd = queries.shape
        cache, nkv = key_cache.shape[0], key_cache.shape[1]
        ratio = nq // nkv
        heads = nkv // 2
        half = nz // 2
        rank = lax.axis_index("cp")
        c = rank % 2
        rows, keys = 2 * tok * ratio, 2 * cache
        dma = pltpu.SemaphoreType.DMA
        out, lse = pl.pallas_call(
            functools.partial(_attend, nz, tok, heads, ratio, cache),
            out_shape=(jax.ShapeDtypeStruct((tok, nq, hd), BF16), jax.ShapeDtypeStruct((2, 8, rows), F32)),
            in_specs=[pl.BlockSpec(memory_space=pl.ANY)] * 5 + [pl.BlockSpec(memory_space=pltpu.SMEM)],
            out_specs=[pl.BlockSpec(memory_space=pl.ANY)] * 2,
            scratch_shapes=[
                pltpu.VMEM((heads, keys, hd), BF16), pltpu.VMEM((heads, hd, keys), BF16),
                pltpu.VMEM((2, heads, NEW_PAD, hd), BF16), pltpu.VMEM((2, heads, hd, hd), BF16),
                pltpu.VMEM((heads, half, 4 * tok, ratio, hd), BF16),
                pltpu.VMEM((keys, TILE), F32), pltpu.VMEM((keys, TILE), F32),
                pltpu.VMEM((2, NEW_PAD, TILE), F32), pltpu.VMEM((2, NEW_PAD, TILE), F32),
                pltpu.VMEM((keys, hd), BF16),
                pltpu.VMEM((TILE, TILE), BF16), pltpu.VMEM((TILE, TILE), BF16),
                pltpu.VMEM((heads, half, hd, 2 * rows), BF16), pltpu.VMEM((heads, half, 1, 2 * rows), F32),
                pltpu.VMEM((2, heads, half, hd, rows), BF16), pltpu.VMEM((2, heads, half, 1, rows), F32),
                pltpu.VMEM((heads, 2 * tok, ratio, hd), BF16), pltpu.VMEM((8, rows), F32),
                pltpu.VMEM((cache * nkv, hd), BF16), pltpu.VMEM((cache * nkv, hd), BF16), pltpu.VMEM((CHUNK * nkv, hd), F32), pltpu.VMEM((CHUNK * nkv, hd), F32),
                pltpu.VMEM((heads, cache, hd), BF16), pltpu.VMEM((heads, hd, cache), BF16),
                pltpu.VMEM((2, tok * nkv, hd), BF16), pltpu.VMEM((heads, NEW_PAD, hd), BF16), pltpu.VMEM((heads, hd, hd), BF16),
                dma((2,)), dma((2, heads)), dma((2, heads)), dma((2, 3)),
                dma((heads,)), dma((heads,)), dma((heads,)),
                dma((2, heads, half)), dma((2, heads, half)),
                dma((2, heads, half)), dma((2, heads, half)),
                dma((2, heads, half)), dma((2, heads, half)),
                dma((heads, 3)), dma((3,)),
            ],
            compiler_params=pltpu.CompilerParams(collective_id=0, has_side_effects=True, vmem_limit_bytes=60 * 2**20),
            name="ring_attend",
        )(queries, key_cache.reshape(cache * nkv, hd), value_cache.reshape(cache * nkv, hd),
          key_new.reshape(tok * nkv, hd), value_new.reshape(tok * nkv, hd), prefix_len)
        lse = lse[:, :heads].reshape(nkv, 2, tok, ratio)
        lse = lax.dynamic_index_in_dim(lse, c, axis=1, keepdims=False)
        row_lse = lse.transpose(1, 0, 2).reshape(tok, nq)
        return out, row_lse

    return jax.shard_map(local, mesh=mesh, in_specs=(tok_spec,) * 5 + (P("dp"),), out_specs=(tok_spec, tok_spec), check_vma=False)
```

```python
import functools

import jax
import jax.numpy as jnp
from jax import lax
from jax.experimental import pallas as pl
from jax.experimental.pallas import tpu as pltpu
from jax.sharding import PartitionSpec as P

NEG = -1e30
LOG2E = 1.4426950408889634
F32 = jnp.float32
BF16 = jnp.bfloat16
TILE = 256
NEW_PAD = 32
SUB = 4096
CHUNK = 128


def _attend(nz, tok, heads, ratio, cache,
            q_hbm, k_hbm, v_hbm, kn_hbm, vn_hbm, plen_ref, out_hbm, lse_hbm,
            kbuf, vbuf, knbuf, vnbuf, qbuf, s0, s1, sn0, sn1, bias, qt0, qt1,
            po, plse, rb, rl, outb, lseb, rawk, rawv, st0, st1, ksend, vsend, rawn, knsend, vnsend,
            raw_sem, kv_send, kv_recv, kn_sem, q_loc, q_send, q_recv,
            ag_send, ag_recv, ro_send, ro_recv, rs_send, rs_recv, out_sem, fin_sem):
    hd = q_hbm.shape[-1]
    scale = hd ** -0.5
    csc = scale * LOG2E
    half = nz // 2
    rows = 2 * tok * ratio
    mine = tok * ratio
    keys = 2 * cache
    per_step = 2 * rows // TILE
    steps = heads * half
    tiles = steps * per_step
    bodies = tiles // 2

    rank = lax.axis_index("cp")
    z, c = rank // 2, rank % 2
    partner = 2 * z + (1 - c)
    right = 2 * lax.rem(z + 1, nz) + c
    left = 2 * lax.rem(z + nz - 1, nz) + c
    to = (right, left)

    barrier = pltpu.get_barrier_semaphore()
    for dev in (partner, right, left):
        pl.semaphore_signal(barrier, inc=1, device_id={"cp": dev}, device_id_type=pl.DeviceIdType.MESH)
    pl.semaphore_wait(barrier, 3)

    def remote(src, dst, ss, rs, dev):
        return pltpu.make_async_remote_copy(src_ref=src, dst_ref=dst, send_sem=ss, recv_sem=rs,
                                            device_id={"cp": dev}, device_id_type=pl.DeviceIdType.MESH)

    def head_rows(ref, n):
        return ref.at[:, pl.ds(pl.multiple_of(n * ratio, ratio), ratio), :]

    def q_in(h):
        dst = qbuf.at[h, 0, pl.ds(c * tok, tok)]
        there = remote(head_rows(q_hbm, heads * (1 - c) + h), dst, q_send.at[h], q_recv.at[h], partner)
        here = pltpu.make_async_copy(head_rows(q_hbm, heads * c + h), dst, q_loc.at[h])
        return there, here

    def raw_in():
        return [pltpu.make_async_copy(src, dst, raw_sem.at[n]) for n, (src, dst) in enumerate(((k_hbm, rawk), (v_hbm, rawv)))]

    def kv_in(h):
        return [remote(ksend.at[h], kbuf.at[h, pl.ds(c * cache, cache), :], kv_send.at[0, h], kv_recv.at[0, h], partner),
                remote(vsend.at[h], vbuf.at[h, :, pl.ds(c * cache, cache)], kv_send.at[1, h], kv_recv.at[1, h], partner)]

    def relayout(raw, put):
        def chunk(i, st):
            st[...] = raw[pl.ds(pl.multiple_of(i * CHUNK * 2 * heads, CHUNK * 2 * heads), CHUNK * 2 * heads), :].astype(F32)
            ok = rank * cache + i * CHUNK + lax.broadcasted_iota(jnp.int32, (CHUNK, hd), 0) < plen_ref[0]
            at0 = pl.multiple_of(i * CHUNK, CHUNK)
            for h in range(heads):
                for own, n in ((True, heads * c + h), (False, heads * (1 - c) + h)):
                    put(own, h, at0, jnp.where(ok, st[pl.ds(n, CHUNK, stride=2 * heads), :], 0.0))

        def two(i, _):
            chunk(2 * i, st0)
            chunk(2 * i + 1, st1)
            return 0
        lax.fori_loop(0, cache // (2 * CHUNK), two, 0)

    def put_k(own, h, at0, x):
        if own:
            kbuf[h, pl.ds(pl.multiple_of(c * cache + at0, CHUNK), CHUNK), :] = x.astype(BF16)
        else:
            ksend[h, pl.ds(at0, CHUNK), :] = x.astype(BF16)

    def put_v(own, h, at0, x):
        if own:
            vbuf[h, :, pl.ds(pl.multiple_of(c * cache + at0, CHUNK), CHUNK)] = x.T.astype(BF16)
        else:
            vsend[h, :, pl.ds(at0, CHUNK)] = x.T.astype(BF16)

    def new_raw():
        return [pltpu.make_async_copy(src, rawn.at[n], kn_sem.at[n, 2]) for n, src in enumerate((kn_hbm, vn_hbm))]

    def new_in():
        return [remote(src, dst.at[c], kn_sem.at[n, 0], kn_sem.at[n, 1], partner)
                for n, (src, dst) in enumerate(((knsend, knbuf), (vnsend, vnbuf)))]

    def relayout_new():
        for n, (pad, mine, theirs) in enumerate(((NEW_PAD, knbuf, knsend), (hd, vnbuf, vnsend))):
            st0[0:tok * 2 * heads, :] = rawn[n].astype(F32)
            for h in range(heads):
                for own, src in ((True, heads * c + h), (False, heads * (1 - c) + h)):
                    x = st0[pl.ds(src, tok, stride=2 * heads), :]
                    x = jnp.concatenate([x, jnp.zeros((pad - tok, hd), F32)], axis=0)
                    x = (x if n == 0 else x.T).astype(BF16)
                    if own:
                        mine[c, h] = x
                    else:
                        theirs[h] = x

    def q_slot(h, d, k):
        if k == 0:
            return qbuf.at[h, 0, pl.ds(0, 2 * tok)]
        if k == half:
            return qbuf.at[h, 0, pl.ds(2 * tok, 2 * tok)]
        return qbuf.at[h, k, pl.ds(d * 2 * tok, 2 * tok)]

    def far_dir(h):
        return h % 2

    def ag(h, d, k):
        return remote(q_slot(h, d, k), q_slot(h, d, k + 1), ag_send.at[d, h, k], ag_recv.at[d, h, k], to[d])

    def ag_start(h, k):
        for d in (0, 1):
            if k + 1 < half or far_dir(h) == d:
                ag(h, d, k).start()

    def ag_wait(h, k):
        for d in (0, 1):
            if k + 1 < half or far_dir(h) == d:
                ag(h, d, k).wait_recv()

    def hop(h, k):
        ag_wait(h, k)
        if k + 1 < half:
            ag_start(h, k + 1)

    def po_part(h, d, k):
        if k == half:
            sl = pl.ds(rows, rows)
            return po.at[h, 0, :, sl], plse.at[h, 0, :, sl]
        sl = pl.ds((1 - d) * rows, rows)
        return po.at[h, k, :, sl], plse.at[h, k, :, sl]

    def rs(h, d, k):
        o, l = po_part(h, d, k)
        return (remote(o, rb.at[d, h, k - 1], ro_send.at[d, h, k - 1], ro_recv.at[d, h, k - 1], to[d]),
                remote(l, rl.at[d, h, k - 1], rs_send.at[d, h, k - 1], rs_recv.at[d, h, k - 1], to[d]))

    def merge(parts):
        top = functools.reduce(jnp.maximum, [l for _, l in parts])
        ws = [jnp.exp(l - top) for _, l in parts]
        tot = functools.reduce(jnp.add, ws)
        inv = 1.0 / tot
        acc = functools.reduce(jnp.add, [o.astype(F32) * (w * inv) for (o, _), w in zip(parts, ws)])
        return acc, top + jnp.log(tot)

    def rs_stage(h, k):
        for d in (0, 1):
            if k == half and far_dir(h) != d:
                continue
            if k + 1 < half or (k + 1 == half and far_dir(h) == d):
                for cp in rs(h, d, k + 1):
                    cp.wait_recv()
                o, l = po_part(h, d, k)
                acc, lse = merge([(o[...], l[...]), (rb[d, h, k], rl[d, h, k])])
                o[...] = acc.astype(BF16)
                l[...] = lse
            for cp in rs(h, d, k):
                cp.start()

    def out_copies(h):
        dst = head_rows(out_hbm, heads * c + h)
        there = remote(outb.at[h, pl.ds((1 - c) * tok, tok)], dst, out_sem.at[h, 0], out_sem.at[h, 1], partner)
        here = pltpu.make_async_copy(outb.at[h, pl.ds(c * tok, tok)], dst, out_sem.at[h, 2])
        return there, here

    def final(h):
        for d in (0, 1):
            for cp in rs(h, d, 1):
                cp.wait_recv()
        acc, lse = merge([(po[h, 0, :, 0:rows], plse[h, 0, :, 0:rows])] + [(rb[d, h, 0], rl[d, h, 0]) for d in (0, 1)])
        outb[h] = acc.T.reshape(2 * tok, ratio, hd).astype(BF16)
        lseb[h:h + 1, :] = lse
        for cp in out_copies(h):
            cp.start()

    def kv_wait(h):
        for there in kv_in(h):
            there.wait_recv()

    def kv_wait_one(h, n):
        kv_in(h)[n].wait_recv()

    for h in range(heads):
        for cp in q_in(h):
            cp.start()
    for cp in raw_in():
        cp.start()
    for cp in new_raw():
        cp.start()

    def q_wait_send(h):
        there, here = q_in(h)
        here.wait()
        there.wait_recv()
        ag_start(h, 0)

    pos = z * keys + lax.broadcasted_iota(jnp.int32, (keys, hd), 0)
    lane = lax.broadcasted_iota(jnp.int32, (keys, hd), 1)
    bias[...] = jnp.where((pos >= plen_ref[0]) & (lane == 0), NEG, 0.0).astype(BF16)
    ones = jnp.where(lax.broadcasted_iota(jnp.int32, (TILE - hd, TILE), 0) == 0, 1.0, 0.0).astype(BF16)
    for r in (qt0, qt1):
        r[hd:TILE, :] = ones
    lseb[...] = jnp.zeros_like(lseb)
    QT, SR, SN = (qt0, qt1), (s0, s1), (sn0, sn1)

    for h in (0, 1):
        q_wait_send(h)
    for cp in new_raw():
        cp.wait()
    relayout_new()
    for cp in new_in():
        cp.start()
    raw_in()[0].wait()
    relayout(rawk, put_k)
    for h in range(heads):
        kv_in(h)[0].start()
    hop(0, 0)
    raw_in()[1].wait()
    relayout(rawv, put_v)
    for h in range(heads):
        kv_in(h)[1].start()

    ev = {i: [] for i in range(bodies + 1)}

    def at(i, f, *a):
        ev[min(i, bodies)].append((f, a))

    table = {
        0: [(hop, 1, 0), (q_wait_send, 2)], 1: [(q_wait_send, 3)], 2: [(hop, 0, 1), (hop, 1, 1)],
        4: [(hop, 3, 0)], 5: [(hop, 2, 0), (hop, 0, 2)], 6: [(hop, 1, 2)], 7: [(hop, 2, 1)],
        8: [(hop, 0, 3), (hop, 1, 3), (hop, 3, 1)], 9: [(hop, 2, 2)], 10: [(hop, 3, 2)],
        11: [(hop, 2, 3), (rs_stage, 0, 4)], 12: [(hop, 3, 3), (rs_stage, 1, 4)], 13: [(rs_stage, 0, 3)],
        14: [(rs_stage, 1, 3), (rs_stage, 2, 4)], 15: [(rs_stage, 3, 4), (rs_stage, 0, 2)], 17: [(rs_stage, 2, 3)],
        18: [(rs_stage, 3, 3), (rs_stage, 0, 1), (rs_stage, 1, 2)], 20: [(rs_stage, 2, 2)], 21: [(rs_stage, 3, 2), (final, 0)],
        22: [(rs_stage, 1, 1)], 23: [(rs_stage, 2, 1)],
        24: [(rs_stage, 3, 1), (final, 1), (final, 2), (final, 3)],
    }
    for i, fs in table.items():
        for f, *a in fs:
            at(i, f, *a)
    at(0, kv_wait, 1)
    at(11, kv_wait, 2)
    at(11, kv_wait, 3)

    def place(t):
        s, n = t // per_step, lax.rem(t, per_step)
        g = s // (2 * half)
        h = 2 * g + lax.rem(s, 2)
        r = (s - 2 * half * g) // 2
        pair = jnp.where(g == 0, lax.rem(r + 1, half), lax.rem(half - r, half))
        return h, pair, n

    def make_qt(t, slot):
        h, pair, n = place(jnp.clip(t, 0, tiles - 1))
        q = qbuf[h, pair, pl.ds(n * (TILE // ratio), TILE // ratio)].astype(F32).reshape(TILE, hd)
        QT[slot][0:hd, :] = q.T.astype(BF16)

    def dot(a, b):
        return lax.dot_general(a, b, (((1,), (0,)), ((), ())), preferred_element_type=F32)

    def colmax(x):
        return jnp.max(x.reshape(x.shape[0] // 8, 8, TILE), axis=0)

    def colsum(x):
        return jnp.sum(x.reshape(x.shape[0] // 8, 8, TILE), axis=0)

    def scores(t, par, mm, u):
        h, pair, n = place(jnp.clip(t, 0, tiles - 1))
        sl = pl.ds(u * SUB, SUB)
        lhs = jnp.concatenate([kbuf[h, sl, :], bias[sl, :]], axis=1)
        if u == 0:
            kn = jnp.concatenate([knbuf[0, h], knbuf[1, h]], axis=0)
            lhs = jnp.concatenate([lhs, jnp.concatenate([kn, jnp.zeros((2 * NEW_PAD, TILE - hd), BF16)], axis=1)], axis=0)
        sv = dot(lhs, QT[par][...])
        if u == 0:
            blk_a = jnp.where(pair == 0, z, lax.rem(z + nz - pair, nz))
            blk_b = jnp.where(pair == 0, lax.rem(z + half, nz), lax.rem(z + pair, nz))
            tl = lax.shift_right_logical(n * TILE + lax.broadcasted_iota(jnp.int32, (NEW_PAD, TILE), 1), ratio.bit_length() - 1)
            last = jnp.where(tl < 2 * tok, 2 * tok * (blk_a - z) + tl, 2 * tok * (blk_b - z - 1) + tl)
            kid = lax.broadcasted_iota(jnp.int32, (NEW_PAD, TILE), 0)
            for q in (0, 1):
                x = jnp.where((kid < tok) & (kid + tok * q <= last), sv[SUB + q * NEW_PAD:SUB + (q + 1) * NEW_PAD], NEG)
                SN[par][q] = x
                mm = jnp.maximum(mm, colmax(x))
            sv = sv[:SUB]
        SR[par][sl, :] = sv
        return jnp.maximum(mm, colmax(sv))

    def tile(i, mm, par):
        h, pair, n = place(i)
        m = jnp.max(mm, axis=0, keepdims=True)
        mc = m * csc
        mm = jnp.full((8, TILE), -jnp.inf, F32)
        l = jnp.zeros((8, TILE), F32)
        pn = []
        for q in (0, 1):
            pe = jnp.exp2(SN[1 - par][q] * csc - mc)
            l = l + colsum(pe)
            pn += [pe.astype(BF16), jnp.zeros((128 - NEW_PAD, TILE), BF16)]
        acc = dot(jnp.concatenate([vnbuf[0, h], vnbuf[1, h]], axis=1), jnp.concatenate(pn, axis=0))
        for u in range(keys // SUB):
            sl = pl.ds(u * SUB, SUB)
            pe = jnp.exp2(SR[1 - par][sl, :] * csc - mc)
            l = l + colsum(pe)
            acc = acc + dot(vbuf[h, :, sl], pe.astype(BF16))
            mm = scores(i + 1, par, mm, u)
        make_qt(i + 2, 1 - par)
        lt = jnp.sum(l, axis=0, keepdims=True)
        sl = pl.ds(pl.multiple_of(n * TILE, TILE), TILE)
        plse[h, pair, :, sl] = m * scale + jnp.log(lt)
        po[h, pair, :, sl] = (acc * (1.0 / lt)).astype(BF16)
        return mm

    kv_wait_one(0, 0)
    for cp in new_in():
        cp.wait_recv()
    make_qt(0, 0)
    first = jnp.full((8, TILE), -jnp.inf, F32)
    for u in range(keys // SUB):
        first = scores(0, 0, first, u)
    make_qt(1, 1)
    kv_wait_one(0, 1)
    for f, a in ev[0]:
        f(*a)

    def pair_of_tiles(t, mm):
        for i in range(1, bodies):
            if ev[i]:
                @pl.when(t == i)
                def _(i=i):
                    for f, a in ev[i]:
                        f(*a)
        return tile(2 * t + 1, tile(2 * t, mm, 1), 0)

    lax.fori_loop(0, bodies, pair_of_tiles, first)

    for f, a in ev[bodies]:
        f(*a)
    fin = (remote(lseb, lse_hbm.at[c], fin_sem.at[0], fin_sem.at[1], partner),
           pltpu.make_async_copy(lseb, lse_hbm.at[c], fin_sem.at[2]))
    for cp in fin:
        cp.start()

    for h in range(heads):
        q_in(h)[0].wait_send()
        for there in kv_in(h):
            there.wait_send()
        for d in (0, 1):
            for k in range(half):
                if k + 1 < half or far_dir(h) == d:
                    ag(h, d, k).wait_send()
            for k in range(1, half + 1):
                if k < half or far_dir(h) == d:
                    for cp in rs(h, d, k):
                        cp.wait_send()
        there, here = out_copies(h)
        here.wait()
        there.wait()
    for cp in new_in():
        cp.wait_send()
    fin[1].wait()
    fin[0].wait()


def solution(mesh):
    nz = mesh.shape["cp"] // 2
    tok_spec = P(("dp", "cp"))

    def local(queries, key_new, value_new, key_cache, value_cache, prefix_len):
        tok, nq, hd = queries.shape
        cache, nkv = key_cache.shape[0], key_cache.shape[1]
        ratio = nq // nkv
        heads = nkv // 2
        half = nz // 2
        rank = lax.axis_index("cp")
        c = rank % 2
        rows, keys = 2 * tok * ratio, 2 * cache
        dma = pltpu.SemaphoreType.DMA
        out, lse = pl.pallas_call(
            functools.partial(_attend, nz, tok, heads, ratio, cache),
            out_shape=(jax.ShapeDtypeStruct((tok, nq, hd), BF16), jax.ShapeDtypeStruct((2, 8, rows), F32)),
            in_specs=[pl.BlockSpec(memory_space=pl.ANY)] * 5 + [pl.BlockSpec(memory_space=pltpu.SMEM)],
            out_specs=[pl.BlockSpec(memory_space=pl.ANY)] * 2,
            scratch_shapes=[
                pltpu.VMEM((heads, keys, hd), BF16), pltpu.VMEM((heads, hd, keys), BF16),
                pltpu.VMEM((2, heads, NEW_PAD, hd), BF16), pltpu.VMEM((2, heads, hd, hd), BF16),
                pltpu.VMEM((heads, half, 4 * tok, ratio, hd), BF16),
                pltpu.VMEM((keys, TILE), F32), pltpu.VMEM((keys, TILE), F32),
                pltpu.VMEM((2, NEW_PAD, TILE), F32), pltpu.VMEM((2, NEW_PAD, TILE), F32),
                pltpu.VMEM((keys, hd), BF16),
                pltpu.VMEM((TILE, TILE), BF16), pltpu.VMEM((TILE, TILE), BF16),
                pltpu.VMEM((heads, half, hd, 2 * rows), BF16), pltpu.VMEM((heads, half, 1, 2 * rows), F32),
                pltpu.VMEM((2, heads, half, hd, rows), BF16), pltpu.VMEM((2, heads, half, 1, rows), F32),
                pltpu.VMEM((heads, 2 * tok, ratio, hd), BF16), pltpu.VMEM((8, rows), F32),
                pltpu.VMEM((cache * nkv, hd), BF16), pltpu.VMEM((cache * nkv, hd), BF16), pltpu.VMEM((CHUNK * nkv, hd), F32), pltpu.VMEM((CHUNK * nkv, hd), F32),
                pltpu.VMEM((heads, cache, hd), BF16), pltpu.VMEM((heads, hd, cache), BF16),
                pltpu.VMEM((2, tok * nkv, hd), BF16), pltpu.VMEM((heads, NEW_PAD, hd), BF16), pltpu.VMEM((heads, hd, hd), BF16),
                dma((2,)), dma((2, heads)), dma((2, heads)), dma((2, 3)),
                dma((heads,)), dma((heads,)), dma((heads,)),
                dma((2, heads, half)), dma((2, heads, half)),
                dma((2, heads, half)), dma((2, heads, half)),
                dma((2, heads, half)), dma((2, heads, half)),
                dma((heads, 3)), dma((3,)),
            ],
            compiler_params=pltpu.CompilerParams(collective_id=0, has_side_effects=True, vmem_limit_bytes=60 * 2**20),
            name="ring_attend",
        )(queries, key_cache.reshape(cache * nkv, hd), value_cache.reshape(cache * nkv, hd),
          key_new.reshape(tok * nkv, hd), value_new.reshape(tok * nkv, hd), prefix_len)
        lse = lse[:, :heads].reshape(nkv, 2, tok, ratio)
        lse = lax.dynamic_index_in_dim(lse, c, axis=1, keepdims=False)
        row_lse = lse.transpose(1, 0, 2).reshape(tok, nq)
        return out, row_lse

    return jax.shard_map(local, mesh=mesh, in_specs=(tok_spec,) * 5 + (P("dp"),), out_specs=(tok_spec, tok_spec), check_vma=False)
```

```python
import functools

import jax
import jax.numpy as jnp
from jax import lax
from jax.experimental import pallas as pl
from jax.experimental.pallas import tpu as pltpu
from jax.sharding import PartitionSpec as P

NEG = -1e30
LOG2E = 1.4426950408889634
F32 = jnp.float32
BF16 = jnp.bfloat16
TILE = 256
NEW_PAD = 32
SUB = 4096
CHUNK = 128


def _attend(nz, tok, heads, ratio, cache,
            q_hbm, k_hbm, v_hbm, kn_hbm, vn_hbm, plen_ref, out_hbm, lse_hbm,
            kbuf, vbuf, knbuf, vnbuf, qbuf, s0, s1, sn0, sn1, bias, qt0, qt1,
            po, plse, rb, rl, outb, lseb, rawk, rawv, st0, st1, ksend, vsend, rawn, knsend, vnsend,
            raw_sem, kv_send, kv_recv, kn_sem, q_loc, q_send, q_recv,
            ag_send, ag_recv, ro_send, ro_recv, rs_send, rs_recv, out_sem, fin_sem):
    hd = q_hbm.shape[-1]
    scale = hd ** -0.5
    csc = scale * LOG2E
    half = nz // 2
    rows = 2 * tok * ratio
    mine = tok * ratio
    keys = 2 * cache
    per_step = 2 * rows // TILE
    steps = heads * half
    tiles = steps * per_step
    bodies = tiles // 2

    rank = lax.axis_index("cp")
    z, c = rank // 2, rank % 2
    partner = 2 * z + (1 - c)
    right = 2 * lax.rem(z + 1, nz) + c
    left = 2 * lax.rem(z + nz - 1, nz) + c
    to = (right, left)

    barrier = pltpu.get_barrier_semaphore()
    for dev in (partner, right, left):
        pl.semaphore_signal(barrier, inc=1, device_id={"cp": dev}, device_id_type=pl.DeviceIdType.MESH)
    pl.semaphore_wait(barrier, 3)

    def remote(src, dst, ss, rs, dev):
        return pltpu.make_async_remote_copy(src_ref=src, dst_ref=dst, send_sem=ss, recv_sem=rs,
                                            device_id={"cp": dev}, device_id_type=pl.DeviceIdType.MESH)

    def head_rows(ref, n):
        return ref.at[:, pl.ds(pl.multiple_of(n * ratio, ratio), ratio), :]

    def q_in(h):
        dst = qbuf.at[h, 0, pl.ds(c * tok, tok)]
        there = remote(head_rows(q_hbm, heads * (1 - c) + h), dst, q_send.at[h], q_recv.at[h], partner)
        here = pltpu.make_async_copy(head_rows(q_hbm, heads * c + h), dst, q_loc.at[h])
        return there, here

    def raw_in():
        return [pltpu.make_async_copy(src, dst, raw_sem.at[n]) for n, (src, dst) in enumerate(((k_hbm, rawk), (v_hbm, rawv)))]

    def kv_in(h):
        return [remote(ksend.at[h], kbuf.at[h, pl.ds(c * cache, cache), :], kv_send.at[0, h], kv_recv.at[0, h], partner),
                remote(vsend.at[h], vbuf.at[h, :, pl.ds(c * cache, cache)], kv_send.at[1, h], kv_recv.at[1, h], partner)]

    def relayout(raw, put):
        def chunk(i, st):
            st[...] = raw[pl.ds(pl.multiple_of(i * CHUNK * 2 * heads, CHUNK * 2 * heads), CHUNK * 2 * heads), :].astype(F32)
            ok = rank * cache + i * CHUNK + lax.broadcasted_iota(jnp.int32, (CHUNK, hd), 0) < plen_ref[0]
            at0 = pl.multiple_of(i * CHUNK, CHUNK)
            for h in range(heads):
                for own, n in ((True, heads * c + h), (False, heads * (1 - c) + h)):
                    put(own, h, at0, jnp.where(ok, st[pl.ds(n, CHUNK, stride=2 * heads), :], 0.0))

        def two(i, _):
            chunk(2 * i, st0)
            chunk(2 * i + 1, st1)
            return 0
        lax.fori_loop(0, cache // (2 * CHUNK), two, 0)

    def put_k(own, h, at0, x):
        if own:
            kbuf[h, pl.ds(pl.multiple_of(c * cache + at0, CHUNK), CHUNK), :] = x.astype(BF16)
        else:
            ksend[h, pl.ds(at0, CHUNK), :] = x.astype(BF16)

    def put_v(own, h, at0, x):
        if own:
            vbuf[h, :, pl.ds(pl.multiple_of(c * cache + at0, CHUNK), CHUNK)] = x.T.astype(BF16)
        else:
            vsend[h, :, pl.ds(at0, CHUNK)] = x.T.astype(BF16)

    def new_raw():
        return [pltpu.make_async_copy(src, rawn.at[n], kn_sem.at[n, 2]) for n, src in enumerate((kn_hbm, vn_hbm))]

    def new_in():
        return [remote(src, dst.at[c], kn_sem.at[n, 0], kn_sem.at[n, 1], partner)
                for n, (src, dst) in enumerate(((knsend, knbuf), (vnsend, vnbuf)))]

    def relayout_new():
        for n, (pad, mine, theirs) in enumerate(((NEW_PAD, knbuf, knsend), (hd, vnbuf, vnsend))):
            st0[0:tok * 2 * heads, :] = rawn[n].astype(F32)
            for h in range(heads):
                for own, src in ((True, heads * c + h), (False, heads * (1 - c) + h)):
                    x = st0[pl.ds(src, tok, stride=2 * heads), :]
                    x = jnp.concatenate([x, jnp.zeros((pad - tok, hd), F32)], axis=0)
                    x = (x if n == 0 else x.T).astype(BF16)
                    if own:
                        mine[c, h] = x
                    else:
                        theirs[h] = x

    def q_slot(h, d, k):
        if k == 0:
            return qbuf.at[h, 0, pl.ds(0, 2 * tok)]
        if k == half:
            return qbuf.at[h, 0, pl.ds(2 * tok, 2 * tok)]
        return qbuf.at[h, k, pl.ds(d * 2 * tok, 2 * tok)]

    def far_dir(h):
        return h % 2

    def ag(h, d, k):
        return remote(q_slot(h, d, k), q_slot(h, d, k + 1), ag_send.at[d, h, k], ag_recv.at[d, h, k], to[d])

    def ag_start(h, k):
        for d in (0, 1):
            if k + 1 < half or far_dir(h) == d:
                ag(h, d, k).start()

    def ag_wait(h, k):
        for d in (0, 1):
            if k + 1 < half or far_dir(h) == d:
                ag(h, d, k).wait_recv()

    def hop(h, k):
        ag_wait(h, k)
        if k + 1 < half:
            ag_start(h, k + 1)

    def po_part(h, d, k):
        if k == half:
            sl = pl.ds(rows, rows)
            return po.at[h, 0, :, sl], plse.at[h, 0, :, sl]
        sl = pl.ds((1 - d) * rows, rows)
        return po.at[h, k, :, sl], plse.at[h, k, :, sl]

    def rs(h, d, k):
        o, l = po_part(h, d, k)
        return (remote(o, rb.at[d, h, k - 1], ro_send.at[d, h, k - 1], ro_recv.at[d, h, k - 1], to[d]),
                remote(l, rl.at[d, h, k - 1], rs_send.at[d, h, k - 1], rs_recv.at[d, h, k - 1], to[d]))

    def merge(parts):
        top = functools.reduce(jnp.maximum, [l for _, l in parts])
        ws = [jnp.exp(l - top) for _, l in parts]
        tot = functools.reduce(jnp.add, ws)
        inv = 1.0 / tot
        acc = functools.reduce(jnp.add, [o.astype(F32) * (w * inv) for (o, _), w in zip(parts, ws)])
        return acc, top + jnp.log(tot)

    def rs_stage(h, k):
        sends = [d for d in (0, 1) if k < half or far_dir(h) == d]
        merges = [d for d in sends if k + 1 < half or (k + 1 == half and far_dir(h) == d)]
        for d in merges:
            for cp in rs(h, d, k + 1):
                cp.wait_recv()
        refs = {d: po_part(h, d, k) for d in merges}
        done = {d: merge([(refs[d][0][...], refs[d][1][...]), (rb[d, h, k], rl[d, h, k])]) for d in merges}
        for d in merges:
            refs[d][0][...] = done[d][0].astype(BF16)
            refs[d][1][...] = done[d][1]
        for d in sends:
            for cp in rs(h, d, k):
                cp.start()

    def out_copies(h):
        dst = head_rows(out_hbm, heads * c + h)
        there = remote(outb.at[h, pl.ds((1 - c) * tok, tok)], dst, out_sem.at[h, 0], out_sem.at[h, 1], partner)
        here = pltpu.make_async_copy(outb.at[h, pl.ds(c * tok, tok)], dst, out_sem.at[h, 2])
        return there, here

    def final(h):
        for d in (0, 1):
            for cp in rs(h, d, 1):
                cp.wait_recv()
        acc, lse = merge([(po[h, 0, :, 0:rows], plse[h, 0, :, 0:rows])] + [(rb[d, h, 0], rl[d, h, 0]) for d in (0, 1)])
        outb[h] = acc.T.reshape(2 * tok, ratio, hd).astype(BF16)
        lseb[h:h + 1, :] = lse
        for cp in out_copies(h):
            cp.start()

    def kv_wait(h):
        for there in kv_in(h):
            there.wait_recv()

    def kv_wait_one(h, n):
        kv_in(h)[n].wait_recv()

    for h in range(heads):
        for cp in q_in(h):
            cp.start()
    for cp in raw_in():
        cp.start()
    for cp in new_raw():
        cp.start()

    def q_wait_send(h):
        there, here = q_in(h)
        here.wait()
        there.wait_recv()
        ag_start(h, 0)

    pos = z * keys + lax.broadcasted_iota(jnp.int32, (keys, hd), 0)
    lane = lax.broadcasted_iota(jnp.int32, (keys, hd), 1)
    bias[...] = jnp.where((pos >= plen_ref[0]) & (lane == 0), NEG, 0.0).astype(BF16)
    ones = jnp.where(lax.broadcasted_iota(jnp.int32, (TILE - hd, TILE), 0) == 0, 1.0, 0.0).astype(BF16)
    for r in (qt0, qt1):
        r[hd:TILE, :] = ones
    QT, SR, SN = (qt0, qt1), (s0, s1), (sn0, sn1)

    for h in (0, 1):
        q_wait_send(h)
    for cp in new_raw():
        cp.wait()
    relayout_new()
    for cp in new_in():
        cp.start()
    raw_in()[0].wait()
    relayout(rawk, put_k)
    for h in range(heads):
        kv_in(h)[0].start()
    hop(0, 0)
    raw_in()[1].wait()
    relayout(rawv, put_v)
    for h in range(heads):
        kv_in(h)[1].start()

    ev = {i: [] for i in range(bodies + 1)}

    def at(i, f, *a):
        ev[min(i, bodies)].append((f, a))

    table = {
        0: [(hop, 1, 0), (q_wait_send, 2)], 1: [(q_wait_send, 3)], 2: [(hop, 0, 1), (hop, 1, 1)],
        4: [(hop, 3, 0)], 5: [(hop, 2, 0), (hop, 0, 2)], 6: [(hop, 1, 2)], 7: [(hop, 2, 1)],
        8: [(hop, 0, 3), (hop, 1, 3), (hop, 3, 1)], 9: [(hop, 2, 2)], 10: [(hop, 3, 2)],
        11: [(hop, 2, 3), (rs_stage, 0, 4)], 12: [(hop, 3, 3), (rs_stage, 1, 4)], 13: [(rs_stage, 0, 3)],
        14: [(rs_stage, 1, 3), (rs_stage, 2, 4)], 15: [(rs_stage, 3, 4), (rs_stage, 0, 2)], 17: [(rs_stage, 2, 3)],
        18: [(rs_stage, 3, 3), (rs_stage, 0, 1), (rs_stage, 1, 2)], 20: [(rs_stage, 2, 2)], 21: [(rs_stage, 3, 2), (final, 0)],
        22: [(rs_stage, 1, 1)], 23: [(rs_stage, 2, 1)],
        24: [(rs_stage, 3, 1), (final, 1), (final, 2), (final, 3)],
    }
    for i, fs in table.items():
        for f, *a in fs:
            at(i, f, *a)
    at(0, kv_wait, 1)
    at(11, kv_wait, 2)
    at(11, kv_wait, 3)

    def place(t):
        s, n = t // per_step, lax.rem(t, per_step)
        g = s // (2 * half)
        h = 2 * g + lax.rem(s, 2)
        r = (s - 2 * half * g) // 2
        pair = jnp.where(g == 0, lax.rem(r + 1, half), lax.rem(half - r, half))
        return h, pair, n

    def make_qt(t, slot):
        h, pair, n = place(jnp.clip(t, 0, tiles - 1))
        q = qbuf[h, pair, pl.ds(n * (TILE // ratio), TILE // ratio)].astype(F32).reshape(TILE, hd)
        QT[slot][0:hd, :] = q.T.astype(BF16)

    def dot(a, b):
        return lax.dot_general(a, b, (((1,), (0,)), ((), ())), preferred_element_type=F32)

    def colmax(x):
        return jnp.max(x.reshape(x.shape[0] // 8, 8, TILE), axis=0)

    def colsum(x):
        return jnp.sum(x.reshape(x.shape[0] // 8, 8, TILE), axis=0)

    def scores(t, par, mm, u):
        h, pair, n = place(jnp.clip(t, 0, tiles - 1))
        sl = pl.ds(u * SUB, SUB)
        lhs = jnp.concatenate([kbuf[h, sl, :], bias[sl, :]], axis=1)
        if u == 0:
            kn = jnp.concatenate([knbuf[0, h], knbuf[1, h]], axis=0)
            lhs = jnp.concatenate([lhs, jnp.concatenate([kn, jnp.zeros((2 * NEW_PAD, TILE - hd), BF16)], axis=1)], axis=0)
        sv = dot(lhs, QT[par][...])
        if u == 0:
            blk_a = jnp.where(pair == 0, z, lax.rem(z + nz - pair, nz))
            blk_b = jnp.where(pair == 0, lax.rem(z + half, nz), lax.rem(z + pair, nz))
            tl = lax.shift_right_logical(n * TILE + lax.broadcasted_iota(jnp.int32, (NEW_PAD, TILE), 1), ratio.bit_length() - 1)
            last = jnp.where(tl < 2 * tok, 2 * tok * (blk_a - z) + tl, 2 * tok * (blk_b - z - 1) + tl)
            kid = lax.broadcasted_iota(jnp.int32, (NEW_PAD, TILE), 0)
            for q in (0, 1):
                x = jnp.where((kid < tok) & (kid + tok * q <= last), sv[SUB + q * NEW_PAD:SUB + (q + 1) * NEW_PAD], NEG)
                SN[par][q] = x
                mm = jnp.maximum(mm, colmax(x))
            sv = sv[:SUB]
        SR[par][sl, :] = sv
        return jnp.maximum(mm, colmax(sv))

    def tile(i, mm, par):
        h, pair, n = place(i)
        m = jnp.max(mm, axis=0, keepdims=True)
        mc = m * csc
        mm = jnp.full((8, TILE), -jnp.inf, F32)
        l = jnp.zeros((8, TILE), F32)
        pn = []
        for q in (0, 1):
            pe = jnp.exp2(SN[1 - par][q] * csc - mc)
            l = l + colsum(pe)
            pn += [pe.astype(BF16), jnp.zeros((128 - NEW_PAD, TILE), BF16)]
        acc = dot(jnp.concatenate([vnbuf[0, h], vnbuf[1, h]], axis=1), jnp.concatenate(pn, axis=0))
        for u in range(keys // SUB):
            sl = pl.ds(u * SUB, SUB)
            pe = jnp.exp2(SR[1 - par][sl, :] * csc - mc)
            l = l + colsum(pe)
            acc = acc + dot(vbuf[h, :, sl], pe.astype(BF16))
            mm = scores(i + 1, par, mm, u)
        make_qt(i + 2, 1 - par)
        lt = jnp.sum(l, axis=0, keepdims=True)
        sl = pl.ds(pl.multiple_of(n * TILE, TILE), TILE)
        plse[h, pair, :, sl] = m * scale + jnp.log(lt)
        po[h, pair, :, sl] = (acc * (1.0 / lt)).astype(BF16)
        return mm

    kv_wait_one(0, 0)
    for cp in new_in():
        cp.wait_recv()
    make_qt(0, 0)
    first = jnp.full((8, TILE), -jnp.inf, F32)
    for u in range(keys // SUB):
        first = scores(0, 0, first, u)
    make_qt(1, 1)
    kv_wait_one(0, 1)
    for f, a in ev[0]:
        f(*a)

    def pair_of_tiles(t, mm):
        for i in range(1, bodies):
            if ev[i]:
                @pl.when(t == i)
                def _(i=i):
                    for f, a in ev[i]:
                        f(*a)
        return tile(2 * t + 1, tile(2 * t, mm, 1), 0)

    lax.fori_loop(0, bodies, pair_of_tiles, first)

    for f, a in ev[bodies]:
        f(*a)
    fin = (remote(lseb, lse_hbm.at[c], fin_sem.at[0], fin_sem.at[1], partner),
           pltpu.make_async_copy(lseb, lse_hbm.at[c], fin_sem.at[2]))
    for cp in fin:
        cp.start()

    for h in range(heads):
        q_in(h)[0].wait_send()
        for there in kv_in(h):
            there.wait_send()
        for d in (0, 1):
            for k in range(half):
                if k + 1 < half or far_dir(h) == d:
                    ag(h, d, k).wait_send()
            for k in range(1, half + 1):
                if k < half or far_dir(h) == d:
                    for cp in rs(h, d, k):
                        cp.wait_send()
        there, here = out_copies(h)
        here.wait()
        there.wait()
    for cp in new_in():
        cp.wait_send()
    fin[1].wait()
    fin[0].wait()


def solution(mesh):
    nz = mesh.shape["cp"] // 2
    tok_spec = P(("dp", "cp"))

    def local(queries, key_new, value_new, key_cache, value_cache, prefix_len):
        tok, nq, hd = queries.shape
        cache, nkv = key_cache.shape[0], key_cache.shape[1]
        ratio = nq // nkv
        heads = nkv // 2
        half = nz // 2
        rank = lax.axis_index("cp")
        c = rank % 2
        rows, keys = 2 * tok * ratio, 2 * cache
        dma = pltpu.SemaphoreType.DMA
        out, lse = pl.pallas_call(
            functools.partial(_attend, nz, tok, heads, ratio, cache),
            out_shape=(jax.ShapeDtypeStruct((tok, nq, hd), BF16), jax.ShapeDtypeStruct((2, heads, rows), F32)),
            in_specs=[pl.BlockSpec(memory_space=pl.ANY)] * 5 + [pl.BlockSpec(memory_space=pltpu.SMEM)],
            out_specs=[pl.BlockSpec(memory_space=pl.ANY)] * 2,
            scratch_shapes=[
                pltpu.VMEM((heads, keys, hd), BF16), pltpu.VMEM((heads, hd, keys), BF16),
                pltpu.VMEM((2, heads, NEW_PAD, hd), BF16), pltpu.VMEM((2, heads, hd, hd), BF16),
                pltpu.VMEM((heads, half, 4 * tok, ratio, hd), BF16),
                pltpu.VMEM((keys, TILE), F32), pltpu.VMEM((keys, TILE), F32),
                pltpu.VMEM((2, NEW_PAD, TILE), F32), pltpu.VMEM((2, NEW_PAD, TILE), F32),
                pltpu.VMEM((keys, hd), BF16),
                pltpu.VMEM((TILE, TILE), BF16), pltpu.VMEM((TILE, TILE), BF16),
                pltpu.VMEM((heads, half, hd, 2 * rows), BF16), pltpu.VMEM((heads, half, 1, 2 * rows), F32),
                pltpu.VMEM((2, heads, half, hd, rows), BF16), pltpu.VMEM((2, heads, half, 1, rows), F32),
                pltpu.VMEM((heads, 2 * tok, ratio, hd), BF16), pltpu.VMEM((heads, rows), F32),
                pltpu.VMEM((cache * nkv, hd), BF16), pltpu.VMEM((cache * nkv, hd), BF16), pltpu.VMEM((CHUNK * nkv, hd), F32), pltpu.VMEM((CHUNK * nkv, hd), F32),
                pltpu.VMEM((heads, cache, hd), BF16), pltpu.VMEM((heads, hd, cache), BF16),
                pltpu.VMEM((2, tok * nkv, hd), BF16), pltpu.VMEM((heads, NEW_PAD, hd), BF16), pltpu.VMEM((heads, hd, hd), BF16),
                dma((2,)), dma((2, heads)), dma((2, heads)), dma((2, 3)),
                dma((heads,)), dma((heads,)), dma((heads,)),
                dma((2, heads, half)), dma((2, heads, half)),
                dma((2, heads, half)), dma((2, heads, half)),
                dma((2, heads, half)), dma((2, heads, half)),
                dma((heads, 3)), dma((3,)),
            ],
            compiler_params=pltpu.CompilerParams(collective_id=0, has_side_effects=True, vmem_limit_bytes=60 * 2**20),
            name="ring_attend",
        )(queries, key_cache.reshape(cache * nkv, hd), value_cache.reshape(cache * nkv, hd),
          key_new.reshape(tok * nkv, hd), value_new.reshape(tok * nkv, hd), prefix_len)
        lse = lse.reshape(nkv, 2, tok, ratio)
        lse = lax.dynamic_index_in_dim(lse, c, axis=1, keepdims=False)
        row_lse = lse.transpose(1, 0, 2).reshape(tok, nq)
        return out, row_lse

    return jax.shard_map(local, mesh=mesh, in_specs=(tok_spec,) * 5 + (P("dp"),), out_specs=(tok_spec, tok_spec), check_vma=False)
```

```python
import functools

import jax
import jax.numpy as jnp
from jax import lax
from jax.experimental import pallas as pl
from jax.experimental.pallas import tpu as pltpu
from jax.sharding import PartitionSpec as P

NEG = -1e30
LOG2E = 1.4426950408889634
F32 = jnp.float32
BF16 = jnp.bfloat16
TILE = 256
NEW_PAD = 32
SUB = 4096
CHUNK = 128


def _attend(nz, tok, heads, ratio, cache,
            q_hbm, k_hbm, v_hbm, kn_hbm, vn_hbm, plen_ref, out_hbm, lse_hbm,
            kbuf, vbuf, knbuf, vnbuf, qbuf, s0, s1, sn0, sn1, bias, qt0, qt1,
            po, plse, rb, rl, outb, lseb, rawk, rawv, st0, st1, ksend, vsend, rawn, knsend, vnsend,
            raw_sem, kv_send, kv_recv, kn_sem, q_loc, q_send, q_recv,
            ag_send, ag_recv, ro_send, ro_recv, rs_send, rs_recv, out_sem, fin_sem):
    hd = q_hbm.shape[-1]
    scale = hd ** -0.5
    csc = scale * LOG2E
    half = nz // 2
    rows = 2 * tok * ratio
    mine = tok * ratio
    keys = 2 * cache
    per_step = 2 * rows // TILE
    steps = heads * half
    tiles = steps * per_step
    bodies = tiles // 2

    rank = lax.axis_index("cp")
    z, c = rank // 2, rank % 2
    partner = 2 * z + (1 - c)
    right = 2 * lax.rem(z + 1, nz) + c
    left = 2 * lax.rem(z + nz - 1, nz) + c
    to = (right, left)

    barrier = pltpu.get_barrier_semaphore()
    for dev in (partner, right, left):
        pl.semaphore_signal(barrier, inc=1, device_id={"cp": dev}, device_id_type=pl.DeviceIdType.MESH)
    pl.semaphore_wait(barrier, 3)

    def remote(src, dst, ss, rs, dev):
        return pltpu.make_async_remote_copy(src_ref=src, dst_ref=dst, send_sem=ss, recv_sem=rs,
                                            device_id={"cp": dev}, device_id_type=pl.DeviceIdType.MESH)

    def head_rows(ref, n):
        return ref.at[:, pl.ds(pl.multiple_of(n * ratio, ratio), ratio), :]

    def q_in(h):
        dst = qbuf.at[h, 0, pl.ds(c * tok, tok)]
        there = remote(head_rows(q_hbm, heads * (1 - c) + h), dst, q_send.at[h], q_recv.at[h], partner)
        here = pltpu.make_async_copy(head_rows(q_hbm, heads * c + h), dst, q_loc.at[h])
        return there, here

    def raw_in():
        return [pltpu.make_async_copy(src, dst, raw_sem.at[n]) for n, (src, dst) in enumerate(((k_hbm, rawk), (v_hbm, rawv)))]

    def kv_in(h):
        return [remote(ksend.at[h], kbuf.at[h, pl.ds(c * cache, cache), :], kv_send.at[0, h], kv_recv.at[0, h], partner),
                remote(vsend.at[h], vbuf.at[h, :, pl.ds(c * cache, cache)], kv_send.at[1, h], kv_recv.at[1, h], partner)]

    def relayout(raw, put):
        def chunk(i, st):
            st[...] = raw[pl.ds(pl.multiple_of(i * CHUNK * 2 * heads, CHUNK * 2 * heads), CHUNK * 2 * heads), :].astype(F32)
            ok = rank * cache + i * CHUNK + lax.broadcasted_iota(jnp.int32, (CHUNK, hd), 0) < plen_ref[0]
            at0 = pl.multiple_of(i * CHUNK, CHUNK)
            for h in range(heads):
                for own, n in ((True, heads * c + h), (False, heads * (1 - c) + h)):
                    put(own, h, at0, jnp.where(ok, st[pl.ds(n, CHUNK, stride=2 * heads), :], 0.0))

        def two(i, _):
            chunk(2 * i, st0)
            chunk(2 * i + 1, st1)
            return 0
        lax.fori_loop(0, cache // (2 * CHUNK), two, 0)

    def put_k(own, h, at0, x):
        if own:
            kbuf[h, pl.ds(pl.multiple_of(c * cache + at0, CHUNK), CHUNK), :] = x.astype(BF16)
        else:
            ksend[h, pl.ds(at0, CHUNK), :] = x.astype(BF16)

    def put_v(own, h, at0, x):
        if own:
            vbuf[h, :, pl.ds(pl.multiple_of(c * cache + at0, CHUNK), CHUNK)] = x.T.astype(BF16)
        else:
            vsend[h, :, pl.ds(at0, CHUNK)] = x.T.astype(BF16)

    def new_raw():
        return [pltpu.make_async_copy(src, rawn.at[n], kn_sem.at[n, 2]) for n, src in enumerate((kn_hbm, vn_hbm))]

    def new_in():
        return [remote(src, dst.at[c], kn_sem.at[n, 0], kn_sem.at[n, 1], partner)
                for n, (src, dst) in enumerate(((knsend, knbuf), (vnsend, vnbuf)))]

    def relayout_new():
        for n, (pad, mine, theirs) in enumerate(((NEW_PAD, knbuf, knsend), (hd, vnbuf, vnsend))):
            st0[0:tok * 2 * heads, :] = rawn[n].astype(F32)
            for h in range(heads):
                for own, src in ((True, heads * c + h), (False, heads * (1 - c) + h)):
                    x = st0[pl.ds(src, tok, stride=2 * heads), :]
                    x = jnp.concatenate([x, jnp.zeros((pad - tok, hd), F32)], axis=0)
                    x = (x if n == 0 else x.T).astype(BF16)
                    if own:
                        mine[c, h] = x
                    else:
                        theirs[h] = x

    def q_slot(h, d, k):
        if k == 0:
            return qbuf.at[h, 0, pl.ds(0, 2 * tok)]
        if k == half:
            return qbuf.at[h, 0, pl.ds(2 * tok, 2 * tok)]
        return qbuf.at[h, k, pl.ds(d * 2 * tok, 2 * tok)]

    def far_dir(h):
        return h % 2

    def ag(h, d, k):
        return remote(q_slot(h, d, k), q_slot(h, d, k + 1), ag_send.at[d, h, k], ag_recv.at[d, h, k], to[d])

    def ag_start(h, k):
        for d in (0, 1):
            if k + 1 < half or far_dir(h) == d:
                ag(h, d, k).start()

    def ag_wait(h, k):
        for d in (0, 1):
            if k + 1 < half or far_dir(h) == d:
                ag(h, d, k).wait_recv()

    def hop(h, k):
        ag_wait(h, k)
        if k + 1 < half:
            ag_start(h, k + 1)

    def po_part(h, d, k):
        if k == half:
            sl = pl.ds(rows, rows)
            return po.at[h, 0, :, sl], plse.at[h, 0, :, sl]
        sl = pl.ds((1 - d) * rows, rows)
        return po.at[h, k, :, sl], plse.at[h, k, :, sl]

    def rs(h, d, k):
        o, l = po_part(h, d, k)
        return (remote(o, rb.at[d, h, k - 1], ro_send.at[d, h, k - 1], ro_recv.at[d, h, k - 1], to[d]),
                remote(l, rl.at[d, h, k - 1], rs_send.at[d, h, k - 1], rs_recv.at[d, h, k - 1], to[d]))

    def merge(parts):
        top = functools.reduce(jnp.maximum, [l for _, l in parts])
        ws = [jnp.exp(l - top) for _, l in parts]
        tot = functools.reduce(jnp.add, ws)
        inv = 1.0 / tot
        acc = functools.reduce(jnp.add, [o.astype(F32) * (w * inv) for (o, _), w in zip(parts, ws)])
        return acc, top + jnp.log(tot)

    def rs_stage(h, k):
        for d in (0, 1):
            if k == half and far_dir(h) != d:
                continue
            if k + 1 < half or (k + 1 == half and far_dir(h) == d):
                for cp in rs(h, d, k + 1):
                    cp.wait_recv()
                o, l = po_part(h, d, k)
                acc, lse = merge([(o[...], l[...]), (rb[d, h, k], rl[d, h, k])])
                o[...] = acc.astype(BF16)
                l[...] = lse
            for cp in rs(h, d, k):
                cp.start()

    def out_copies(h):
        dst = head_rows(out_hbm, heads * c + h)
        there = remote(outb.at[h, pl.ds((1 - c) * tok, tok)], dst, out_sem.at[h, 0], out_sem.at[h, 1], partner)
        here = pltpu.make_async_copy(outb.at[h, pl.ds(c * tok, tok)], dst, out_sem.at[h, 2])
        return there, here

    def final(h):
        for d in (0, 1):
            for cp in rs(h, d, 1):
                cp.wait_recv()
        acc, lse = merge([(po[h, 0, :, 0:rows], plse[h, 0, :, 0:rows])] + [(rb[d, h, 0], rl[d, h, 0]) for d in (0, 1)])
        outb[h] = acc.T.reshape(2 * tok, ratio, hd).astype(BF16)
        lseb[h:h + 1, :] = lse
        for cp in out_copies(h):
            cp.start()

    def kv_wait(h):
        for there in kv_in(h):
            there.wait_recv()

    def kv_wait_one(h, n):
        kv_in(h)[n].wait_recv()

    for h in range(heads):
        for cp in q_in(h):
            cp.start()
    for cp in raw_in():
        cp.start()
    for cp in new_raw():
        cp.start()

    def q_wait_send(h):
        there, here = q_in(h)
        here.wait()
        there.wait_recv()
        ag_start(h, 0)

    pos = z * keys + lax.broadcasted_iota(jnp.int32, (keys, hd), 0)
    lane = lax.broadcasted_iota(jnp.int32, (keys, hd), 1)
    bias[...] = jnp.where((pos >= plen_ref[0]) & (lane == 0), NEG, 0.0).astype(BF16)
    ones = jnp.where(lax.broadcasted_iota(jnp.int32, (TILE - hd, TILE), 0) == 0, 1.0, 0.0).astype(BF16)
    for r in (qt0, qt1):
        r[hd:TILE, :] = ones
    QT, SR, SN = (qt0, qt1), (s0, s1), (sn0, sn1)

    for h in (0, 1):
        q_wait_send(h)
    for cp in new_raw():
        cp.wait()
    relayout_new()
    for cp in new_in():
        cp.start()
    raw_in()[0].wait()
    relayout(rawk, put_k)
    for h in range(heads):
        kv_in(h)[0].start()
    hop(0, 0)
    raw_in()[1].wait()
    relayout(rawv, put_v)
    for h in range(heads):
        kv_in(h)[1].start()

    ev = {i: [] for i in range(bodies + 1)}

    def at(i, f, *a):
        ev[min(i, bodies)].append((f, a))

    table = {
        0: [(hop, 1, 0), (q_wait_send, 2)], 1: [(q_wait_send, 3)], 2: [(hop, 0, 1), (hop, 1, 1)],
        4: [(hop, 3, 0)], 5: [(hop, 2, 0), (hop, 0, 2)], 6: [(hop, 1, 2)], 7: [(hop, 2, 1)],
        8: [(hop, 0, 3), (hop, 1, 3), (hop, 3, 1)], 9: [(hop, 2, 2)], 10: [(hop, 3, 2)],
        11: [(hop, 2, 3), (rs_stage, 0, 4)], 12: [(hop, 3, 3), (rs_stage, 1, 4)], 13: [(rs_stage, 0, 3)],
        14: [(rs_stage, 1, 3), (rs_stage, 2, 4)], 15: [(rs_stage, 3, 4), (rs_stage, 0, 2)], 17: [(rs_stage, 2, 3)],
        18: [(rs_stage, 3, 3), (rs_stage, 0, 1), (rs_stage, 1, 2)], 20: [(rs_stage, 2, 2)], 21: [(rs_stage, 3, 2)],
        22: [(rs_stage, 1, 1)], 23: [(rs_stage, 2, 1)],
        24: [(rs_stage, 3, 1), (final, 0), (final, 1), (final, 2), (final, 3)],
    }
    for i, fs in table.items():
        for f, *a in fs:
            at(i, f, *a)
    at(0, kv_wait, 1)
    at(11, kv_wait, 2)
    at(11, kv_wait, 3)

    def place(t):
        s, n = t // per_step, lax.rem(t, per_step)
        g = s // (2 * half)
        h = 2 * g + lax.rem(s, 2)
        r = (s - 2 * half * g) // 2
        pair = jnp.where(g == 0, lax.rem(r + 1, half), lax.rem(half - r, half))
        return h, pair, n

    def make_qt(t, slot):
        h, pair, n = place(jnp.clip(t, 0, tiles - 1))
        q = qbuf[h, pair, pl.ds(n * (TILE // ratio), TILE // ratio)].astype(F32).reshape(TILE, hd)
        QT[slot][0:hd, :] = q.T.astype(BF16)

    def dot(a, b):
        return lax.dot_general(a, b, (((1,), (0,)), ((), ())), preferred_element_type=F32)

    def colmax(x):
        return jnp.max(x.reshape(x.shape[0] // 8, 8, TILE), axis=0)

    def colsum(x):
        return jnp.sum(x.reshape(x.shape[0] // 8, 8, TILE), axis=0)

    def scores(t, par, mm, u):
        h, pair, n = place(jnp.clip(t, 0, tiles - 1))
        sl = pl.ds(u * SUB, SUB)
        lhs = jnp.concatenate([kbuf[h, sl, :], bias[sl, :]], axis=1)
        if u == 0:
            kn = jnp.concatenate([knbuf[0, h], knbuf[1, h]], axis=0)
            lhs = jnp.concatenate([lhs, jnp.concatenate([kn, jnp.zeros((2 * NEW_PAD, TILE - hd), BF16)], axis=1)], axis=0)
        sv = dot(lhs, QT[par][...])
        if u == 0:
            blk_a = jnp.where(pair == 0, z, lax.rem(z + nz - pair, nz))
            blk_b = jnp.where(pair == 0, lax.rem(z + half, nz), lax.rem(z + pair, nz))
            tl = lax.shift_right_logical(n * TILE + lax.broadcasted_iota(jnp.int32, (NEW_PAD, TILE), 1), ratio.bit_length() - 1)
            last = jnp.where(tl < 2 * tok, 2 * tok * (blk_a - z) + tl, 2 * tok * (blk_b - z - 1) + tl)
            kid = lax.broadcasted_iota(jnp.int32, (NEW_PAD, TILE), 0)
            for q in (0, 1):
                x = jnp.where((kid < tok) & (kid + tok * q <= last), sv[SUB + q * NEW_PAD:SUB + (q + 1) * NEW_PAD], NEG)
                SN[par][q] = x
                mm = jnp.maximum(mm, colmax(x))
            sv = sv[:SUB]
        SR[par][sl, :] = sv
        return jnp.maximum(mm, colmax(sv))

    def tile(i, mm, par):
        h, pair, n = place(i)
        m = jnp.max(mm, axis=0, keepdims=True)
        mc = m * csc
        mm = jnp.full((8, TILE), -jnp.inf, F32)
        l = jnp.zeros((8, TILE), F32)
        pn = []
        for q in (0, 1):
            pe = jnp.exp2(SN[1 - par][q] * csc - mc)
            l = l + colsum(pe)
            pn += [pe.astype(BF16), jnp.zeros((128 - NEW_PAD, TILE), BF16)]
        acc = dot(jnp.concatenate([vnbuf[0, h], vnbuf[1, h]], axis=1), jnp.concatenate(pn, axis=0))
        for u in range(keys // SUB):
            sl = pl.ds(u * SUB, SUB)
            pe = jnp.exp2(SR[1 - par][sl, :] * csc - mc)
            l = l + colsum(pe)
            acc = acc + dot(vbuf[h, :, sl], pe.astype(BF16))
            mm = scores(i + 1, par, mm, u)
        make_qt(i + 2, 1 - par)
        lt = jnp.sum(l, axis=0, keepdims=True)
        sl = pl.ds(pl.multiple_of(n * TILE, TILE), TILE)
        plse[h, pair, :, sl] = m * scale + jnp.log(lt)
        po[h, pair, :, sl] = (acc * (1.0 / lt)).astype(BF16)
        return mm

    kv_wait_one(0, 0)
    for cp in new_in():
        cp.wait_recv()
    make_qt(0, 0)
    first = jnp.full((8, TILE), -jnp.inf, F32)
    for u in range(keys // SUB):
        first = scores(0, 0, first, u)
    make_qt(1, 1)
    kv_wait_one(0, 1)
    for f, a in ev[0]:
        f(*a)

    def pair_of_tiles(t, mm):
        for i in range(1, bodies):
            if ev[i]:
                @pl.when(t == i)
                def _(i=i):
                    for f, a in ev[i]:
                        f(*a)
        return tile(2 * t + 1, tile(2 * t, mm, 1), 0)

    lax.fori_loop(0, bodies, pair_of_tiles, first)

    for f, a in ev[bodies]:
        f(*a)
    fin = (remote(lseb, lse_hbm.at[c], fin_sem.at[0], fin_sem.at[1], partner),
           pltpu.make_async_copy(lseb, lse_hbm.at[c], fin_sem.at[2]))
    for cp in fin:
        cp.start()

    for h in range(heads):
        q_in(h)[0].wait_send()
        for there in kv_in(h):
            there.wait_send()
        for d in (0, 1):
            for k in range(half):
                if k + 1 < half or far_dir(h) == d:
                    ag(h, d, k).wait_send()
            for k in range(1, half + 1):
                if k < half or far_dir(h) == d:
                    for cp in rs(h, d, k):
                        cp.wait_send()
        there, here = out_copies(h)
        here.wait()
        there.wait()
    for cp in new_in():
        cp.wait_send()
    fin[1].wait()
    fin[0].wait()


def solution(mesh):
    nz = mesh.shape["cp"] // 2
    tok_spec = P(("dp", "cp"))

    def local(queries, key_new, value_new, key_cache, value_cache, prefix_len):
        tok, nq, hd = queries.shape
        cache, nkv = key_cache.shape[0], key_cache.shape[1]
        ratio = nq // nkv
        heads = nkv // 2
        half = nz // 2
        rank = lax.axis_index("cp")
        c = rank % 2
        rows, keys = 2 * tok * ratio, 2 * cache
        dma = pltpu.SemaphoreType.DMA
        out, lse = pl.pallas_call(
            functools.partial(_attend, nz, tok, heads, ratio, cache),
            out_shape=(jax.ShapeDtypeStruct((tok, nq, hd), BF16), jax.ShapeDtypeStruct((2, heads, rows), F32)),
            in_specs=[pl.BlockSpec(memory_space=pl.ANY)] * 5 + [pl.BlockSpec(memory_space=pltpu.SMEM)],
            out_specs=[pl.BlockSpec(memory_space=pl.ANY)] * 2,
            scratch_shapes=[
                pltpu.VMEM((heads, keys, hd), BF16), pltpu.VMEM((heads, hd, keys), BF16),
                pltpu.VMEM((2, heads, NEW_PAD, hd), BF16), pltpu.VMEM((2, heads, hd, hd), BF16),
                pltpu.VMEM((heads, half, 4 * tok, ratio, hd), BF16),
                pltpu.VMEM((keys, TILE), F32), pltpu.VMEM((keys, TILE), F32),
                pltpu.VMEM((2, NEW_PAD, TILE), F32), pltpu.VMEM((2, NEW_PAD, TILE), F32),
                pltpu.VMEM((keys, hd), BF16),
                pltpu.VMEM((TILE, TILE), BF16), pltpu.VMEM((TILE, TILE), BF16),
                pltpu.VMEM((heads, half, hd, 2 * rows), BF16), pltpu.VMEM((heads, half, 1, 2 * rows), F32),
                pltpu.VMEM((2, heads, half, hd, rows), BF16), pltpu.VMEM((2, heads, half, 1, rows), F32),
                pltpu.VMEM((heads, 2 * tok, ratio, hd), BF16), pltpu.VMEM((heads, rows), F32),
                pltpu.VMEM((cache * nkv, hd), BF16), pltpu.VMEM((cache * nkv, hd), BF16), pltpu.VMEM((CHUNK * nkv, hd), F32), pltpu.VMEM((CHUNK * nkv, hd), F32),
                pltpu.VMEM((heads, cache, hd), BF16), pltpu.VMEM((heads, hd, cache), BF16),
                pltpu.VMEM((2, tok * nkv, hd), BF16), pltpu.VMEM((heads, NEW_PAD, hd), BF16), pltpu.VMEM((heads, hd, hd), BF16),
                dma((2,)), dma((2, heads)), dma((2, heads)), dma((2, 3)),
                dma((heads,)), dma((heads,)), dma((heads,)),
                dma((2, heads, half)), dma((2, heads, half)),
                dma((2, heads, half)), dma((2, heads, half)),
                dma((2, heads, half)), dma((2, heads, half)),
                dma((heads, 3)), dma((3,)),
            ],
            compiler_params=pltpu.CompilerParams(collective_id=0, has_side_effects=True, vmem_limit_bytes=60 * 2**20),
            name="ring_attend",
        )(queries, key_cache.reshape(cache * nkv, hd), value_cache.reshape(cache * nkv, hd),
          key_new.reshape(tok * nkv, hd), value_new.reshape(tok * nkv, hd), prefix_len)
        lse = lse.reshape(nkv, 2, tok, ratio)
        lse = lax.dynamic_index_in_dim(lse, c, axis=1, keepdims=False)
        row_lse = lse.transpose(1, 0, 2).reshape(tok, nq)
        return out, row_lse

    return jax.shard_map(local, mesh=mesh, in_specs=(tok_spec,) * 5 + (P("dp"),), out_specs=(tok_spec, tok_spec), check_vma=False)
```
